256 devices in a mesh: gx: 32 (over z_hi, y, core), gy: 8 (over x, z_lo).
Axes of the slice: x: 4, y: 4, z: 8 (z_hi: 4, z_lo: 2; z = z_hi * 2 + z_lo), core: 2. Of those that a mesh axis runs over, the one named last changes fastest.
Arguments:
- innovation: float32 [2, 1536, 1536], P(None, 'gx', 'gy'), may hold values from -6 to 6
- obs_weight: float32 [2, 1536, 1536], P(None, 'gx', 'gy'), may hold values from 0.2 to 2
- static_scale: float32 [2, 1536, 1536], P(None, 'gx', 'gy'), may hold values from 0.3 to 1.5
- members: bfloat16 [36, 2, 512, 512], P(None, None, ('gx', 'gy')), may hold values from -1 to 1
- diffusivity: bfloat16 [2, 512, 512], P(None, ('gx', 'gy')), may hold values from 0.049804688 to 0.23925781
Outputs:
- increment: float32 [2, 1536, 1536], P(None, 'gx', 'gy')
- static_control: float32 [2, 1536, 1536], P(None, 'gx', 'gy')
The draws below stay inside these ranges and needn't reach their ends.
All inputs are finite; a program needn't handle non-finite values.
Results may differ from the reference program's by a relative error of at most 0.0004.
Values may be sent and summed in bfloat16 or wider, within the bound.
A program may use at most 64 MiB of HBM per device.

```python
import math
import jax
import jax.numpy as jnp
from jax import lax

MEMBERS = 36
LEV = 2
NPASS = 4
ITERS = 3
NXC = 512
NYC = 512
NXF = 1536
NYF = 1536


def levels(key, shape, split, low, top_value):
    loudness, own = 1.0, jax.random.fold_in(key, 6)
    for dim, blocks in split:
        draws = jnp.exp(jax.random.uniform(jax.random.fold_in(own, dim), (blocks,), jnp.float32, low / len(split), top_value / len(split)))
        loudness = loudness * jnp.repeat(draws, shape[dim] // blocks).reshape([-1 if axis == dim else 1 for axis in range(len(shape))])
    return loudness


def normal_values(own_key, dims, scale, most, cuts=(), dtype=jnp.bfloat16):
    drawn = scale * jax.random.normal(own_key, dims, jnp.float32)
    if cuts:
        drawn = drawn * levels(own_key, dims, cuts, -0.22, 0.18)
    return jnp.clip(drawn, -most, most).astype(dtype)


def setup_inputs(seed: int = 0) -> dict:
    key_of = jax.random.split(jax.random.key(seed), 6)
    return {
        "innovation": normal_values(key_of[0], (LEV, NXF, NYF), 1.0, 6.0, ((1, 32), (2, 8)), jnp.float32),
        "obs_weight": jnp.clip(jnp.exp(math.log(2.0) - 2.3025851 * jax.random.uniform(key_of[1], (LEV, NXF, NYF), jnp.float32) ** levels(key_of[1], (LEV, NXF, NYF), ((1, 32), (2, 8)), -0.2, 0.2)), 0.2, 2.0),
        "static_scale": jnp.clip(jnp.exp(math.log(1.5) - 1.60943787 * jax.random.uniform(key_of[2], (LEV, NXF, NYF), jnp.float32) ** levels(key_of[2], (LEV, NXF, NYF), ((1, 32), (2, 8)), -0.2, 0.2)), 0.3, 1.5),
        "members": normal_values(key_of[3], (MEMBERS, LEV, NXC, NYC), 0.17, 1.0, ((2, 256),)),
        "diffusivity": jnp.clip(jnp.exp(math.log(0.23925781) - 1.5694326 * jax.random.uniform(key_of[4], (LEV, NXC, NYC), jnp.float32) ** levels(key_of[4], (LEV, NXC, NYC), ((1, 256),), -0.2, 0.2)), 0.049804688, 0.23925781).astype(jnp.bfloat16),
    }


THIRD = 1.0 / 3.0
TWO_THIRDS = 2.0 / 3.0


def laplace_padded(padded):
    center = padded[..., 1:-1, 1:-1]
    return padded[..., 2:, 1:-1] + padded[..., :-2, 1:-1] + padded[..., 1:-1, 2:] + padded[..., 1:-1, :-2] - 4.0 * center


def zero_pad(values):
    widths = [(0, 0)] * (values.ndim - 2) + [(1, 1), (1, 1)]
    return jnp.pad(values, widths)


def prolong_axis(padded, along):
    length = padded.shape[along] - 2
    lowers = lax.slice_in_dim(padded, 0, length, axis=along)
    middle = lax.slice_in_dim(padded, 1, length + 1, axis=along)
    uppers = lax.slice_in_dim(padded, 2, length + 2, axis=along)
    stacked = jnp.stack([lowers * THIRD + middle * TWO_THIRDS, middle, middle * TWO_THIRDS + uppers * THIRD], axis=along)
    target = list(middle.shape)
    target[along] = 3 * length
    return stacked.reshape(target)


def restrict_axis(padded, along):
    length = padded.shape[along] - 2
    position = padded.ndim + along
    count = length // 3

    def reshaped(start):
        portion = lax.slice_in_dim(padded, start, start + length, axis=along)
        target = list(portion.shape[:position]) + [count, 3] + list(portion.shape[position + 1:])
        return portion.reshape(target)

    left_side = lax.index_in_dim(reshaped(0), 0, position + 1, keepdims=False)
    centred = reshaped(1)
    right_side = lax.index_in_dim(reshaped(2), 2, position + 1, keepdims=False)
    first = lax.index_in_dim(centred, 0, position + 1, keepdims=False)
    second = lax.index_in_dim(centred, 1, position + 1, keepdims=False)
    third = lax.index_in_dim(centred, 2, position + 1, keepdims=False)
    return left_side * THIRD + first * TWO_THIRDS + second + third * TWO_THIRDS + right_side * THIRD


def forward(static_part, amplitude, members, rates, static_scale):
    for repeat in range(NPASS):
        amplitude = amplitude + rates * laplace_padded(zero_pad(amplitude))
    coarse = jnp.sum(members.astype(jnp.float32) * amplitude, axis=0)
    padded = zero_pad(coarse)
    return static_scale * static_part + prolong_axis(prolong_axis(padded, -1), -2)


def adjoint(weighted, members, rates, static_scale):
    padded = zero_pad(weighted)
    coarse = restrict_axis(restrict_axis(padded, -2), -1)
    amplitude = members.astype(jnp.float32) * coarse[None]
    for repeat in range(NPASS):
        amplitude = amplitude + laplace_padded(zero_pad(rates * amplitude))
    return static_scale * weighted, amplitude


def inner(left, right):
    return jnp.sum(left[0] * right[0]) + jnp.sum(left[1] * right[1])


def advance(first, scale, second):
    return (first[0] + scale * second[0], first[1] + scale * second[1])


def reference(innovation, obs_weight, static_scale, members, diffusivity):
    rates = diffusivity.astype(jnp.float32)

    def hessian(control):
        pushed = forward(control[0], control[1], members, rates, static_scale)
        back = adjoint(obs_weight * pushed, members, rates, static_scale)
        return (control[0] + back[0], control[1] + back[1]), pushed

    right_hand = adjoint(obs_weight * innovation, members, rates, static_scale)
    control = (jnp.zeros_like(right_hand[0]), jnp.zeros_like(right_hand[1]))
    increment = jnp.zeros_like(innovation)
    residual = right_hand
    direction = right_hand
    norm_now = inner(residual, residual)
    for repeat in range(ITERS):
        curved, pushed = hessian(direction)
        step_size = norm_now / inner(direction, curved)
        control = advance(control, step_size, direction)
        increment = increment + step_size * pushed
        residual = advance(residual, -step_size, curved)
        norm_next = inner(residual, residual)
        direction = advance(residual, norm_next / norm_now, direction)
        norm_now = norm_next
    return increment, control[0]
```

```python
import functools

import jax
import jax.numpy as jnp
from jax import lax
from jax.experimental import pallas as pl
from jax.experimental.pallas import tpu as pltpu
from jax.sharding import PartitionSpec as P

TR, TC, FR, FC = 16, 64, 48, 192
HR, HC, ER = 10, 32, 36
PAIRS = ER // 2
NPASS = 4
F32, BF16 = jnp.float32, jnp.bfloat16
MESH = pl.DeviceIdType.MESH
NINE = 1.0 / 9.0


def iota(shape, dim):
    return lax.broadcasted_iota(jnp.int32, shape, dim)


def weight(fine, coarse):
    return jnp.maximum(3 - jnp.abs(fine - 3 * coarse - 1), 0)


def parts(x):
    high = x.astype(BF16)
    rest = x - high.astype(F32)
    mid = rest.astype(BF16)
    low = (rest - mid.astype(F32)).astype(BF16)
    return high, mid, low


def dot_left(const, x):
    return functools.reduce(jnp.add, [jnp.dot(const, p, preferred_element_type=F32) for p in parts(x)])


def dot_right(x, const):
    return functools.reduce(jnp.add, [jnp.dot(p, const, preferred_element_type=F32) for p in parts(x)])


def diffuse(x, q, k, first):
    n = x.shape[0] - 2
    mid = x[1:-1]
    around = (x[2:] + x[:-2]) + (pltpu.roll(mid, 1, 2) + pltpu.roll(mid, 127, 2))
    return q[first + 1 : first + 1 + n] * mid + k[first + 1 : first + 1 + n] * around


def kernel(
    NX, NY, innov, wobs, sscale, source,
    inc_ref, stat_ref,
    mbuf, kbuf, qbuf, ibuf, kc, acc, cbuf, rows_w, cols_w, prows_w, pcols_w,
    snd_c, snd_n, snd_s, rcv_c, rcv_n, rcv_s,
    vq, vb, red_own, red_y, red_own2, red_x,
    m_send, m_recv, m_local, h_send, h_recv, c_send, c_recv, ry_send, ry_recv, rx_send, rx_recv,
):
    gx, gy = lax.axis_index("gx"), lax.axis_index("gy")
    north, south = lax.rem(gx + NX - 1, NX), lax.rem(gx + 1, NX)
    west, east = lax.rem(gy + NY - 1, NY), lax.rem(gy + 1, NY)

    barrier = pltpu.get_barrier_semaphore()
    for d in range(1, NY):
        pl.semaphore_signal(barrier, inc=1, device_id=(gx, lax.rem(gy + d, NY)), device_id_type=MESH)

    def greet(d, _):
        pl.semaphore_signal(barrier, inc=1, device_id=(lax.rem(gx + d, NX), gy), device_id_type=MESH)
        return 0

    lax.fori_loop(1, NX, greet, 0)
    for row in (north, south):
        for col in (west, east):
            pl.semaphore_signal(barrier, inc=1, device_id=(row, col), device_id_type=MESH)

    has_n = jnp.where(gx > 0, 1, 0)
    has_s = jnp.where(gx < NX - 1, 1, 0)
    has_w = jnp.where(gy > 0, 1, 0)
    has_e = jnp.where(gy < NY - 1, 1, 0)
    for b, on in ((0, has_w), (1, 1), (2, has_e)):
        shape = (FC, 128)
        cell = iota(shape, 1) - HC + TC * (b - 1)
        cols_w[:, 128 * b : 128 * (b + 1)] = (weight(iota(shape, 0), cell) * on).astype(F32).astype(BF16)
    for start, count, shift, on in ((0, 24, -2, 1), (48, 16, -2, has_n), (80, 16, 6, has_s)):
        shape = (count, 2 * FR)
        for lev in range(2):
            fine = iota(shape, 1) - FR * lev
            value = jnp.where((fine >= 0) & (fine < FR), weight(fine, iota(shape, 0) + shift) * on, 0)
            rows_w[start + count * lev : start + count * (lev + 1), :] = value.astype(F32)
    shape = (2 * FR, (TR + 2) * 8)
    lev_of = jnp.where(iota(shape, 0) >= FR, 1, 0)
    inner = iota(shape, 1)
    value = jnp.where((inner & 1) == lev_of, weight(iota(shape, 0) - FR * lev_of, (inner >> 3) - 1), 0)
    prows_w[...] = value.astype(F32).astype(BF16)
    shape = (128, FC)
    pcols_w[...] = weight(iota(shape, 1), iota(shape, 0) - HC).astype(F32).astype(BF16)

    def c_copies(app):
        found = []
        for b, col in ((0, west), (1, gy), (2, east)):
            for kind, (row, snd, rcv) in enumerate(((gx, snd_c, rcv_c), (north, snd_n, rcv_n), (south, snd_s, rcv_s))):
                if b == 1 and kind == 0:
                    continue
                found.append(
                    pltpu.make_async_remote_copy(
                        src_ref=snd.at[app, b], dst_ref=rcv.at[app, b],
                        send_sem=c_send.at[app, kind, b], recv_sem=c_recv.at[app, kind, b],
                        device_id=(row, col), device_id_type=MESH,
                    )
                )
        return found

    def restrict(app, v):
        wide = dot_right(v, cols_w[...])
        z = dot_left(rows_w[...].astype(BF16), wide) * NINE
        for b in range(3):
            snd_c[app, b] = z[0:48, 128 * b : 128 * (b + 1)]
            snd_n[app, b] = z[48:80, 128 * b : 128 * (b + 1)]
            snd_s[app, b] = z[80:112, 128 * b : 128 * (b + 1)]

    first = wobs[...] * innov[...]
    vq[0] = first
    restrict(0, first)

    pl.semaphore_wait(barrier, (NY - 1) + (NX - 1) + 4)

    for copy in c_copies(0):
        copy.start()

    moves = []
    for d in range(1, NY):
        col = lax.rem(gy + d, NY)
        moves.append(
            pltpu.make_async_remote_copy(
                src_ref=source.at[col], dst_ref=mbuf.at[gy + 5],
                send_sem=m_send.at[d], recv_sem=m_recv.at[d],
                device_id=(gx, col), device_id_type=MESH,
            )
        )
    for copy in moves:
        copy.start()
    own = pltpu.make_async_copy(source.at[gy], mbuf.at[gy + 5], m_local)
    own.start()
    own.wait()
    for copy in moves:
        copy.wait_recv()
    halos = [
        pltpu.make_async_remote_copy(
            src_ref=mbuf.at[pl.ds(begin, 5)], dst_ref=mbuf.at[pl.ds(to, 5)],
            send_sem=h_send.at[i], recv_sem=h_recv.at[i], device_id=(row, gy), device_id_type=MESH,
        )
        for i, (begin, to, row) in enumerate(((5, 13, north), (8, 0, south)))
    ]
    for copy in halos:
        copy.start()
    for copy in halos:
        copy.wait_recv()

    row_of = iota((ER, 8, 128), 0)
    inside = jnp.where(((row_of >= HR) | (gx > 0)) & ((row_of < HR + TR) | (gx < NX - 1)), 1.0, 0.0)
    rate = mbuf[:, 9].astype(F32).reshape(ER, 8, 128) * inside
    kbuf[...] = rate
    qbuf[...] = 1.0 - 4.0 * rate
    ibuf[...] = jnp.where(rate > 0.0, 1.0 / jnp.where(rate > 0.0, rate, 1.0), 0.0)

    lev_odd = (iota((8, 128), 0) & 1) == 1

    def apply(app, v):
        for copy in c_copies(app):
            copy.wait_recv()
        mine = snd_c[app, 1] + rcv_c[app, 0] + rcv_c[app, 2]
        north_in = rcv_s[app, 0] + rcv_s[app, 1] + rcv_s[app, 2]
        south_in = rcv_n[app, 0] + rcv_n[app, 1] + rcv_n[app, 2]
        for lev in range(2):
            c, n, s = mine[24 * lev : 24 * lev + 24], north_in[16 * lev : 16 * lev + 16], south_in[16 * lev : 16 * lev + 16]
            cbuf[lev, 0:8] = n[0:8]
            cbuf[lev, 8:16] = n[8:16] + c[0:8]
            cbuf[lev, 16:24] = c[8:16]
            cbuf[lev, 24:32] = c[16:24] + s[0:8]
            cbuf[lev, 32:40] = s[8:16]
        for e in range(1, ER - 1):
            even = jnp.broadcast_to(cbuf[0, e : e + 1, :], (8, 128))
            odd = jnp.broadcast_to(cbuf[1, e : e + 1, :], (8, 128))
            kc[e] = jnp.where(lev_odd, odd, even) * kbuf[e]
        acc[...] = jnp.zeros_like(acc)

        def chunk(ch, _):
            m = mbuf[:, ch].astype(F32).reshape(ER, 8, 128)
            x = m[1 : ER - 1] * kc[1 : ER - 1]
            at = 1
            for repeat in range(NPASS):
                x = diffuse(x, qbuf, kbuf, at)
                at += 1
            x = x * ibuf[at : at + x.shape[0]]
            for repeat in range(NPASS):
                x = diffuse(x, qbuf, kbuf, at)
                at += 1
            acc[...] += x * m[at : ER - at]
            return 0

        lax.fori_loop(0, 9, chunk, 0)
        tall = dot_left(prows_w[...], acc[...].reshape((TR + 2) * 8, 128))
        scale = sscale[...]
        return scale * scale * v + dot_right(tall, pcols_w[...]) * NINE

    lane = iota((1, 128), 1)

    def pack(pairs):
        out = jnp.zeros((1, 128), F32)
        for i, (left, right) in enumerate(pairs):
            total = jnp.sum(jnp.sum(left * right, axis=0, keepdims=True), axis=1, keepdims=True)
            out = jnp.where(lane == i, total, out)
        return out

    def y_copy(use, d):
        return pltpu.make_async_remote_copy(
            src_ref=red_own.at[use], dst_ref=red_y.at[use, d], send_sem=ry_send.at[use, d], recv_sem=ry_recv.at[use, d],
            device_id=(gx, lax.rem(gy + d, NY)), device_id_type=MESH,
        )

    def x_copy(use, d):
        return pltpu.make_async_remote_copy(
            src_ref=red_own2.at[use], dst_ref=red_x.at[use, d], send_sem=rx_send.at[use, d], recv_sem=rx_recv.at[use, d],
            device_id=(lax.rem(gx + d, NX), gy), device_id_type=MESH,
        )

    def each(count, make, what):
        def body(d, _):
            getattr(make(d), what)()
            return 0

        lax.fori_loop(1, count, body, 0)

    def reduce_start(use, row):
        red_own[use] = row
        each(NY, functools.partial(y_copy, use), "start")

    def reduce_middle(use):
        each(NY, functools.partial(y_copy, use), "wait_recv")
        total = red_own[use]
        for d in range(1, NY):
            total = total + red_y[use, d]
        red_own2[use] = total
        each(NX, functools.partial(x_copy, use), "start")

    def reduce_end(use):
        each(NX, functools.partial(x_copy, use), "wait_recv")
        total = red_own2[use]
        for d in range(1, NX):
            total = total + red_x[use, d]
        each(NY, functools.partial(y_copy, use), "wait_send")
        each(NX, functools.partial(x_copy, use), "wait_send")
        return total

    def pick(row, i):
        return jnp.sum(jnp.where(lane == i, row, 0.0), axis=1, keepdims=True)

    w = wobs[...]
    b0 = apply(0, vq[0])
    vb[0] = b0
    q1 = w * b0
    restrict(1, q1)
    for copy in c_copies(1):
        copy.start()
    reduce_start(0, pack(((vq[0], b0), (q1, b0))))
    vq[1] = q1
    reduce_middle(0)
    b1 = apply(1, vq[1])
    sums = reduce_end(0)
    theta = pick(sums, 1) / pick(sums, 0)
    b1 = b1 - theta * vb[0]
    vq[1] = vq[1] - theta * vq[0]
    vb[1] = b1
    q2 = w * b1
    restrict(2, q2)
    for copy in c_copies(2):
        copy.start()
    vq[2] = q2
    b2 = apply(2, vq[2])
    vb[2] = b2
    q0, q1, b0, b1 = vq[0], vq[1], vb[0], vb[1]
    wb = (w * b0, w * b1, w * b2)
    q2 = vq[2]
    row = pack((
        (q0, b0), (q0, b1), (q0, b2), (q1, b1), (q1, b2), (q2, b2),
        (b0, wb[0]), (b0, wb[1]), (b0, wb[2]), (b1, wb[1]), (b1, wb[2]), (b2, wb[2]),
    ))
    reduce_start(1, row)
    reduce_middle(1)
    sums = reduce_end(1)
    e = [pick(sums, i) for i in range(12)]
    s00, s01, s02, s11, s12, s22 = [e[i] + e[6 + i] for i in range(6)]
    tiny = 1e-7
    i0 = 1.0 / s00
    l10, l20 = s01 * i0, s02 * i0
    d1 = s11 - l10 * s01
    i1 = jnp.where(d1 > tiny * s11, 1.0 / d1, 0.0)
    t12 = s12 - l10 * s02
    l21 = t12 * i1
    d2 = s22 - l20 * s02 - l21 * t12
    i2 = jnp.where(d2 > tiny * s22, 1.0 / d2, 0.0)
    r0, r1, r2 = e[0], e[1], e[2]
    r1 = r1 - l10 * r0
    r2 = r2 - l20 * r0 - l21 * r1
    z2 = r2 * i2
    z1 = r1 * i1 - l21 * z2
    z0 = r0 * i0 - l10 * z1 - l20 * z2
    inc_ref[...] = z0 * vb[0] + z1 * vb[1] + z2 * vb[2]
    stat_ref[...] = sscale[...] * (z0 * vq[0] + z1 * vq[1] + z2 * vq[2])

    for app in range(3):
        for copy in c_copies(app):
            copy.wait_send()
    for copy in moves:
        copy.wait_send()
    for copy in halos:
        copy.wait_send()


def per_device(NX, NY, innovation, obs_weight, static_scale, members, diffusivity):
    wide = members.shape[-1]
    m = members.reshape(9, 4, 2, 2, wide).transpose(0, 3, 1, 2, 4).reshape(9, 16, wide)
    k = jnp.broadcast_to(diffusivity.transpose(1, 0, 2)[:, None], (2, 4, 2, wide)).reshape(1, 16, wide)
    both = jnp.pad(jnp.concatenate([m, k]), ((0, 0), (0, 0), (HC, 128 - TC - HC)))
    source = jnp.stack([both[:, :, TC * j : TC * j + 128] for j in range(NY)])
    vec = (2 * FR, FC)
    vmem = pl.BlockSpec(memory_space=pltpu.VMEM)
    dma = pltpu.SemaphoreType.DMA
    inc, stat = pl.pallas_call(
        functools.partial(kernel, NX, NY),
        out_shape=(jax.ShapeDtypeStruct(vec, F32), jax.ShapeDtypeStruct(vec, F32)),
        in_specs=[vmem] * 4,
        out_specs=(vmem, vmem),
        scratch_shapes=[
            pltpu.VMEM((PAIRS, 10, 16, 128), BF16),
            pltpu.VMEM((ER, 8, 128), F32),
            pltpu.VMEM((ER, 8, 128), F32),
            pltpu.VMEM((ER, 8, 128), F32),
            pltpu.VMEM((ER, 8, 128), F32),
            pltpu.VMEM((TR + 2, 8, 128), F32),
            pltpu.VMEM((2, 40, 128), F32),
            pltpu.VMEM((112, 2 * FR), F32),
            pltpu.VMEM((FC, 384), BF16),
            pltpu.VMEM((2 * FR, (TR + 2) * 8), BF16),
            pltpu.VMEM((128, FC), BF16),
            pltpu.VMEM((3, 3, 48, 128), F32),
            pltpu.VMEM((3, 3, 32, 128), F32),
            pltpu.VMEM((3, 3, 32, 128), F32),
            pltpu.VMEM((3, 3, 48, 128), F32),
            pltpu.VMEM((3, 3, 32, 128), F32),
            pltpu.VMEM((3, 3, 32, 128), F32),
            pltpu.VMEM((3,) + vec, F32),
            pltpu.VMEM((3,) + vec, F32),
            pltpu.VMEM((2, 1, 128), F32),
            pltpu.VMEM((2, NY, 1, 128), F32),
            pltpu.VMEM((2, 1, 128), F32),
            pltpu.VMEM((2, NX, 1, 128), F32),
            dma((NY,)), dma((NY,)), dma,
            dma((2,)), dma((2,)),
            dma((3, 3, 3)), dma((3, 3, 3)),
            dma((2, NY)), dma((2, NY)),
            dma((2, NX)), dma((2, NX)),
        ],
        compiler_params=pltpu.CompilerParams(collective_id=0, has_side_effects=True),
        name="solve",
    )(innovation.reshape(vec), obs_weight.reshape(vec), static_scale.reshape(vec), source)
    return inc.reshape(2, FR, FC), stat.reshape(2, FR, FC)


def solution(mesh):
    NX, NY = mesh.shape["gx"], mesh.shape["gy"]
    fine = P(None, "gx", "gy")
    return jax.shard_map(
        functools.partial(per_device, NX, NY),
        mesh=mesh,
        in_specs=(fine, fine, fine, P(None, None, ("gx", "gy"), None), P(None, ("gx", "gy"), None)),
        out_specs=(fine, fine),
        check_vma=False,
    )
```

```python
import functools

import jax
import jax.numpy as jnp
from jax import lax
from jax.experimental import pallas as pl
from jax.experimental.pallas import tpu as pltpu
from jax.sharding import PartitionSpec as P

TR, TC, FR, FC = 16, 64, 48, 192
HR, HC, ER = 10, 32, 36
PAIRS = ER // 2
NPASS = 4
F32, BF16 = jnp.float32, jnp.bfloat16
MESH = pl.DeviceIdType.MESH
NINE = 1.0 / 9.0


def iota(shape, dim):
    return lax.broadcasted_iota(jnp.int32, shape, dim)


def weight(fine, coarse):
    return jnp.maximum(3 - jnp.abs(fine - 3 * coarse - 1), 0)


def parts(x):
    high = x.astype(BF16)
    rest = x - high.astype(F32)
    mid = rest.astype(BF16)
    low = (rest - mid.astype(F32)).astype(BF16)
    return high, mid, low


def dot_left(const, x):
    return functools.reduce(jnp.add, [jnp.dot(const, p, preferred_element_type=F32) for p in parts(x)])


def dot_right(x, const):
    return functools.reduce(jnp.add, [jnp.dot(p, const, preferred_element_type=F32) for p in parts(x)])


def diffuse(row, store, center, around, first, last):
    above, here = row(first - 1), row(first)
    for r in range(first, last):
        below = row(r + 1)
        near = (above + below) + (pltpu.roll(here, 1, 2) + pltpu.roll(here, 127, 2))
        store(r, center[r][None] * here + around[r][None] * near)
        above, here = here, below


def kernel(
    NX, NY, innov, wobs, sscale, source,
    inc_ref, stat_ref,
    mbuf, mf, xa, xb, kbuf, qbuf, ibuf, rbuf, kc, acc, cbuf, rows_w, cols_w, prows_w, pcols_w,
    snd_c, snd_n, snd_s, rcv_c, rcv_n, rcv_s,
    vq, vb, red_own, red_y, red_own2, red_x,
    m_send, m_recv, m_local, h_send, h_recv, c_send, c_recv, ry_send, ry_recv, rx_send, rx_recv,
):
    gx, gy = lax.axis_index("gx"), lax.axis_index("gy")
    north, south = lax.rem(gx + NX - 1, NX), lax.rem(gx + 1, NX)
    west, east = lax.rem(gy + NY - 1, NY), lax.rem(gy + 1, NY)

    barrier = pltpu.get_barrier_semaphore()
    for d in range(1, NY):
        pl.semaphore_signal(barrier, inc=1, device_id=(gx, lax.rem(gy + d, NY)), device_id_type=MESH)

    def greet(d, _):
        pl.semaphore_signal(barrier, inc=1, device_id=(lax.rem(gx + d, NX), gy), device_id_type=MESH)
        return 0

    lax.fori_loop(1, NX, greet, 0)
    for row in (north, south):
        for col in (west, east):
            pl.semaphore_signal(barrier, inc=1, device_id=(row, col), device_id_type=MESH)

    has_n = jnp.where(gx > 0, 1, 0)
    has_s = jnp.where(gx < NX - 1, 1, 0)
    has_w = jnp.where(gy > 0, 1, 0)
    has_e = jnp.where(gy < NY - 1, 1, 0)
    for b, on in ((0, has_w), (1, 1), (2, has_e)):
        shape = (FC, 128)
        cell = iota(shape, 1) - HC + TC * (b - 1)
        cols_w[:, 128 * b : 128 * (b + 1)] = (weight(iota(shape, 0), cell) * on).astype(F32).astype(BF16)
    for start, count, shift, on in ((0, 24, -2, 1), (48, 16, -2, has_n), (80, 16, 6, has_s)):
        shape = (count, 2 * FR)
        for lev in range(2):
            fine = iota(shape, 1) - FR * lev
            value = jnp.where((fine >= 0) & (fine < FR), weight(fine, iota(shape, 0) + shift) * on, 0)
            rows_w[start + count * lev : start + count * (lev + 1), :] = value.astype(F32)
    shape = (2 * FR, (TR + 2) * 8)
    lev_of = jnp.where(iota(shape, 0) >= FR, 1, 0)
    inner = iota(shape, 1)
    value = jnp.where((inner & 1) == lev_of, weight(iota(shape, 0) - FR * lev_of, (inner >> 3) - 1), 0)
    prows_w[...] = value.astype(F32).astype(BF16)
    shape = (128, FC)
    pcols_w[...] = weight(iota(shape, 1), iota(shape, 0) - HC).astype(F32).astype(BF16)

    def c_copies(app):
        found = []
        for b, col in ((0, west), (1, gy), (2, east)):
            for kind, (row, snd, rcv) in enumerate(((gx, snd_c, rcv_c), (north, snd_n, rcv_n), (south, snd_s, rcv_s))):
                if b == 1 and kind == 0:
                    continue
                found.append(
                    pltpu.make_async_remote_copy(
                        src_ref=snd.at[app, b], dst_ref=rcv.at[app, b],
                        send_sem=c_send.at[app, kind, b], recv_sem=c_recv.at[app, kind, b],
                        device_id=(row, col), device_id_type=MESH,
                    )
                )
        return found

    def restrict(app, v):
        wide = dot_right(v, cols_w[...])
        z = dot_left(rows_w[...].astype(BF16), wide) * NINE
        for b in range(3):
            snd_c[app, b] = z[0:48, 128 * b : 128 * (b + 1)]
            snd_n[app, b] = z[48:80, 128 * b : 128 * (b + 1)]
            snd_s[app, b] = z[80:112, 128 * b : 128 * (b + 1)]

    first = wobs[...] * innov[...]
    vq[0] = first
    restrict(0, first)

    pl.semaphore_wait(barrier, (NY - 1) + (NX - 1) + 4)

    for copy in c_copies(0):
        copy.start()

    moves = []
    for d in range(1, NY):
        col = lax.rem(gy + d, NY)
        moves.append(
            pltpu.make_async_remote_copy(
                src_ref=source.at[col], dst_ref=mbuf.at[gy + 5],
                send_sem=m_send.at[d], recv_sem=m_recv.at[d],
                device_id=(gx, col), device_id_type=MESH,
            )
        )
    for copy in moves:
        copy.start()
    own = pltpu.make_async_copy(source.at[gy], mbuf.at[gy + 5], m_local)
    own.start()

    def halo(side, d):
        g = lax.rem(gy + NY - d, NY)
        return g <= 4 if side == 0 else g >= 3, pltpu.make_async_remote_copy(
            src_ref=source.at[gy] if d == 0 else mbuf.at[g + 5],
            dst_ref=mbuf.at[jnp.minimum(g, 4) + 13 if side == 0 else jnp.maximum(g, 3) - 3],
            send_sem=h_send.at[side, d], recv_sem=h_recv.at[side, d],
            device_id=(north if side == 0 else south, gy), device_id_type=MESH,
        )

    def halo_do(d, what):
        for side in range(2):
            used, copy = halo(side, d)

            @pl.when(used)
            def _():
                getattr(copy, what)()

    halo_do(0, "start")
    for d in range(1, NY):
        moves[d - 1].wait_recv()
        halo_do(d, "start")
    own.wait()
    for d in range(NY):
        halo_do(d, "wait_recv")

    row_of = iota((ER, 8, 128), 0)
    inside = jnp.where(((row_of >= HR) | (gx > 0)) & ((row_of < HR + TR) | (gx < NX - 1)), 1.0, 0.0)
    rate = mbuf[:, 9].astype(F32).reshape(ER, 8, 128) * inside
    kbuf[...] = rate
    qbuf[...] = 1.0 - 4.0 * rate
    known = rate > 0.0
    ibuf[...] = jnp.where(known, 1.0, 0.0)
    rbuf[...] = jnp.where(known, 1.0 / jnp.where(known, rate, 1.0) - 4.0, 0.0)
    for ch in range(9):
        mf[:, ch] = mbuf[:, ch].astype(F32).reshape(ER, 8, 128)

    lev_odd = (iota((8, 128), 0) & 1) == 1

    def apply(app, v):
        for copy in c_copies(app):
            copy.wait_recv()
        mine = snd_c[app, 1] + rcv_c[app, 0] + rcv_c[app, 2]
        north_in = rcv_s[app, 0] + rcv_s[app, 1] + rcv_s[app, 2]
        south_in = rcv_n[app, 0] + rcv_n[app, 1] + rcv_n[app, 2]
        for lev in range(2):
            c, n, s = mine[24 * lev : 24 * lev + 24], north_in[16 * lev : 16 * lev + 16], south_in[16 * lev : 16 * lev + 16]
            cbuf[lev, 0:8] = n[0:8]
            cbuf[lev, 8:16] = n[8:16] + c[0:8]
            cbuf[lev, 16:24] = c[8:16]
            cbuf[lev, 24:32] = c[16:24] + s[0:8]
            cbuf[lev, 32:40] = s[8:16]
        for e in range(1, ER - 1):
            even = jnp.broadcast_to(cbuf[0, e : e + 1, :], (8, 128))
            odd = jnp.broadcast_to(cbuf[1, e : e + 1, :], (8, 128))
            kc[e] = jnp.where(lev_odd, odd, even) * kbuf[e]
        bufs = (xa, xb)
        for p in range(2 * NPASS):
            src, dst = bufs[p % 2], bufs[(p + 1) % 2]
            row = (lambda r: mf[r] * kc[r][None]) if p == 0 else (lambda r, src=src: src[r])

            def store(r, x, dst=dst, p=p):
                if p == 2 * NPASS - 1:
                    acc[r - (HR - 1)] = jnp.sum(x * mf[r], axis=0)
                else:
                    dst[r] = x

            middle = p == NPASS - 1
            diffuse(row, store, rbuf if middle else qbuf, ibuf if middle else kbuf, 2 + p, ER - 2 - p)
        tall = dot_left(prows_w[...], acc[...].reshape((TR + 2) * 8, 128))
        scale = sscale[...]
        return scale * scale * v + dot_right(tall, pcols_w[...]) * NINE

    lane = iota((1, 128), 1)

    def pack(pairs):
        out = jnp.zeros((1, 128), F32)
        for i, (left, right) in enumerate(pairs):
            total = jnp.sum(jnp.sum(left * right, axis=0, keepdims=True), axis=1, keepdims=True)
            out = jnp.where(lane == i, total, out)
        return out

    def y_copy(use, d):
        return pltpu.make_async_remote_copy(
            src_ref=red_own.at[use], dst_ref=red_y.at[use, d], send_sem=ry_send.at[use, d], recv_sem=ry_recv.at[use, d],
            device_id=(gx, lax.rem(gy + d, NY)), device_id_type=MESH,
        )

    def x_copy(use, d):
        return pltpu.make_async_remote_copy(
            src_ref=red_own2.at[use], dst_ref=red_x.at[use, d], send_sem=rx_send.at[use, d], recv_sem=rx_recv.at[use, d],
            device_id=(lax.rem(gx + d, NX), gy), device_id_type=MESH,
        )

    def each(count, make, what):
        def body(d, _):
            getattr(make(d), what)()
            return 0

        lax.fori_loop(1, count, body, 0)

    def reduce_start(use, row):
        red_own[use] = row
        each(NY, functools.partial(y_copy, use), "start")

    def reduce_middle(use):
        each(NY, functools.partial(y_copy, use), "wait_recv")
        total = red_own[use]
        for d in range(1, NY):
            total = total + red_y[use, d]
        red_own2[use] = total
        each(NX, functools.partial(x_copy, use), "start")

    def reduce_end(use):
        each(NX, functools.partial(x_copy, use), "wait_recv")
        total = red_own2[use]
        for d in range(1, NX):
            total = total + red_x[use, d]
        each(NY, functools.partial(y_copy, use), "wait_send")
        each(NX, functools.partial(x_copy, use), "wait_send")
        return total

    def pick(row, i):
        return jnp.sum(jnp.where(lane == i, row, 0.0), axis=1, keepdims=True)

    w = wobs[...]
    b0 = apply(0, vq[0])
    vb[0] = b0
    q1 = w * b0
    restrict(1, q1)
    for copy in c_copies(1):
        copy.start()
    reduce_start(0, pack(((vq[0], b0), (q1, b0))))
    vq[1] = q1
    reduce_middle(0)
    b1 = apply(1, vq[1])
    sums = reduce_end(0)
    theta = pick(sums, 1) / pick(sums, 0)
    b1 = b1 - theta * vb[0]
    vq[1] = vq[1] - theta * vq[0]
    vb[1] = b1
    q2 = w * b1
    restrict(2, q2)
    for copy in c_copies(2):
        copy.start()
    vq[2] = q2
    b2 = apply(2, vq[2])
    vb[2] = b2
    q0, q1, b0, b1 = vq[0], vq[1], vb[0], vb[1]
    wb = (w * b0, w * b1, w * b2)
    q2 = vq[2]
    row = pack((
        (q0, b0), (q0, b1), (q0, b2), (q1, b1), (q1, b2), (q2, b2),
        (b0, wb[0]), (b0, wb[1]), (b0, wb[2]), (b1, wb[1]), (b1, wb[2]), (b2, wb[2]),
    ))
    reduce_start(1, row)
    reduce_middle(1)
    sums = reduce_end(1)
    e = [pick(sums, i) for i in range(12)]
    s00, s01, s02, s11, s12, s22 = [e[i] + e[6 + i] for i in range(6)]
    tiny = 1e-7
    i0 = 1.0 / s00
    l10, l20 = s01 * i0, s02 * i0
    d1 = s11 - l10 * s01
    i1 = jnp.where(d1 > tiny * s11, 1.0 / d1, 0.0)
    t12 = s12 - l10 * s02
    l21 = t12 * i1
    d2 = s22 - l20 * s02 - l21 * t12
    i2 = jnp.where(d2 > tiny * s22, 1.0 / d2, 0.0)
    r0, r1, r2 = e[0], e[1], e[2]
    r1 = r1 - l10 * r0
    r2 = r2 - l20 * r0 - l21 * r1
    z2 = r2 * i2
    z1 = r1 * i1 - l21 * z2
    z0 = r0 * i0 - l10 * z1 - l20 * z2
    inc_ref[...] = z0 * vb[0] + z1 * vb[1] + z2 * vb[2]
    stat_ref[...] = sscale[...] * (z0 * vq[0] + z1 * vq[1] + z2 * vq[2])

    for app in range(3):
        for copy in c_copies(app):
            copy.wait_send()
    for copy in moves:
        copy.wait_send()
    for d in range(NY):
        halo_do(d, "wait_send")


def per_device(NX, NY, innovation, obs_weight, static_scale, members, diffusivity):
    wide = members.shape[-1]
    m = members.reshape(9, 4, 2, 2, wide).transpose(0, 3, 1, 2, 4).reshape(9, 16, wide)
    k = jnp.broadcast_to(diffusivity.transpose(1, 0, 2)[:, None], (2, 4, 2, wide)).reshape(1, 16, wide)
    both = jnp.pad(jnp.concatenate([m, k]), ((0, 0), (0, 0), (HC, 128 - TC - HC)))
    source = jnp.stack([both[:, :, TC * j : TC * j + 128] for j in range(NY)])
    vec = (2 * FR, FC)
    vmem = pl.BlockSpec(memory_space=pltpu.VMEM)
    dma = pltpu.SemaphoreType.DMA
    inc, stat = pl.pallas_call(
        functools.partial(kernel, NX, NY),
        out_shape=(jax.ShapeDtypeStruct(vec, F32), jax.ShapeDtypeStruct(vec, F32)),
        in_specs=[vmem] * 4,
        out_specs=(vmem, vmem),
        scratch_shapes=[
            pltpu.VMEM((PAIRS, 10, 16, 128), BF16),
            pltpu.VMEM((ER, 9, 8, 128), F32),
            pltpu.VMEM((ER, 9, 8, 128), F32),
            pltpu.VMEM((ER, 9, 8, 128), F32),
            pltpu.VMEM((ER, 8, 128), F32),
            pltpu.VMEM((ER, 8, 128), F32),
            pltpu.VMEM((ER, 8, 128), F32),
            pltpu.VMEM((ER, 8, 128), F32),
            pltpu.VMEM((ER, 8, 128), F32),
            pltpu.VMEM((TR + 2, 8, 128), F32),
            pltpu.VMEM((2, 40, 128), F32),
            pltpu.VMEM((112, 2 * FR), F32),
            pltpu.VMEM((FC, 384), BF16),
            pltpu.VMEM((2 * FR, (TR + 2) * 8), BF16),
            pltpu.VMEM((128, FC), BF16),
            pltpu.VMEM((3, 3, 48, 128), F32),
            pltpu.VMEM((3, 3, 32, 128), F32),
            pltpu.VMEM((3, 3, 32, 128), F32),
            pltpu.VMEM((3, 3, 48, 128), F32),
            pltpu.VMEM((3, 3, 32, 128), F32),
            pltpu.VMEM((3, 3, 32, 128), F32),
            pltpu.VMEM((3,) + vec, F32),
            pltpu.VMEM((3,) + vec, F32),
            pltpu.VMEM((2, 1, 128), F32),
            pltpu.VMEM((2, NY, 1, 128), F32),
            pltpu.VMEM((2, 1, 128), F32),
            pltpu.VMEM((2, NX, 1, 128), F32),
            dma((NY,)), dma((NY,)), dma,
            dma((2, NY)), dma((2, NY)),
            dma((3, 3, 3)), dma((3, 3, 3)),
            dma((2, NY)), dma((2, NY)),
            dma((2, NX)), dma((2, NX)),
        ],
        compiler_params=pltpu.CompilerParams(collective_id=0, has_side_effects=True),
        name="solve",
    )(innovation.reshape(vec), obs_weight.reshape(vec), static_scale.reshape(vec), source)
    return inc.reshape(2, FR, FC), stat.reshape(2, FR, FC)


def solution(mesh):
    NX, NY = mesh.shape["gx"], mesh.shape["gy"]
    fine = P(None, "gx", "gy")
    return jax.shard_map(
        functools.partial(per_device, NX, NY),
        mesh=mesh,
        in_specs=(fine, fine, fine, P(None, None, ("gx", "gy"), None), P(None, ("gx", "gy"), None)),
        out_specs=(fine, fine),
        check_vma=False,
    )
```

```python
import functools

import jax
import jax.numpy as jnp
from jax import lax
from jax.experimental import pallas as pl
from jax.experimental.pallas import tpu as pltpu
from jax.sharding import PartitionSpec as P

TR, TC, FR, FC = 16, 64, 48, 192
HR, HC, ER, POS = 10, 9, 36, 28
MSG = 112
PAIRS = ER // 2
NPASS = 4
F32, BF16 = jnp.float32, jnp.bfloat16
MESH = pl.DeviceIdType.MESH
NINE = 1.0 / 9.0


def iota(shape, dim):
    return lax.broadcasted_iota(jnp.int32, shape, dim)


def weight(fine, coarse):
    return jnp.maximum(3 - jnp.abs(fine - 3 * coarse - 1), 0)


def parts(x):
    high = x.astype(BF16)
    rest = x - high.astype(F32)
    mid = rest.astype(BF16)
    low = (rest - mid.astype(F32)).astype(BF16)
    return high, mid, low


def dot_left(const, x):
    return functools.reduce(jnp.add, [jnp.dot(const, p, preferred_element_type=F32) for p in parts(x)])


def dot_right(x, const):
    return functools.reduce(jnp.add, [jnp.dot(p, const, preferred_element_type=F32) for p in parts(x)])


def diffuse(row, store, center, around, first, last):
    above, here = row(first - 1), row(first)
    for r in range(first, last):
        below = row(r + 1)
        for p in range(3):
            before = here[p - 1] if p else pltpu.roll(here[2], 1, 2)
            after = here[p + 1] if p < 2 else pltpu.roll(here[0], 127, 2)
            near = (above[p] + below[p]) + (before + after)
            store(r, p, center[r, p][None] * here[p] + around[r, p][None] * near)
        above, here = here, below


def kernel(
    NX, NY, innov, wobs, sscale, raw,
    inc_ref, stat_ref,
    mbuf, mf, xa, xb, kbuf, qbuf, ibuf, rbuf, kc, acc, cbuf, cw, kw, kcomp, stage, source, unpacked,
    rows_w, cols_w, prows_w, pcols_w, spread_w,
    snd_c, snd_n, snd_s, rcv_c, rcv_n, rcv_s,
    vq, vb, red_own, red_y, red_own2, red_x,
    m_send, m_recv, m_local, h_send, h_recv, c_send, c_recv, ry_send, ry_recv, rx_send, rx_recv,
):
    gx, gy = lax.axis_index("gx"), lax.axis_index("gy")
    north, south = lax.rem(gx + NX - 1, NX), lax.rem(gx + 1, NX)
    west, east = lax.rem(gy + NY - 1, NY), lax.rem(gy + 1, NY)

    barrier = pltpu.get_barrier_semaphore()
    for d in sorted(range(1, NX), key=lambda d: min(d % 8, 8 - d % 8), reverse=True):
        pl.semaphore_signal(barrier, inc=1, device_id=(lax.rem(gx + d, NX), gy), device_id_type=MESH)
    for row in (north, south):
        for col in (west, east):
            pl.semaphore_signal(barrier, inc=1, device_id=(row, col), device_id_type=MESH)
    for d in range(1, NY):
        pl.semaphore_signal(barrier, inc=1, device_id=(gx, lax.rem(gy + d, NY)), device_id_type=MESH)

    has_n = jnp.where(gx > 0, 1, 0)
    has_s = jnp.where(gx < NX - 1, 1, 0)
    has_w = jnp.where(gy > 0, 1, 0)
    has_e = jnp.where(gy < NY - 1, 1, 0)
    for b, on in ((0, has_w), (1, 1), (2, has_e)):
        shape = (FC, 128)
        at = iota(shape, 1)
        cell = 3 * (at & 31) + (at >> 5) - HC + TC * (b - 1)
        value = jnp.where(((at & 31) < POS) & (at < 96), weight(iota(shape, 0), cell) * on, 0)
        cols_w[:, 128 * b : 128 * (b + 1)] = value.astype(F32).astype(BF16)
    for start, count, shift, on in ((0, 24, -2, 1), (48, 16, -2, has_n), (80, 16, 6, has_s)):
        shape = (count, 2 * FR)
        for lev in range(2):
            fine = iota(shape, 1) - FR * lev
            value = jnp.where((fine >= 0) & (fine < FR), weight(fine, iota(shape, 0) + shift) * on, 0)
            rows_w[start + count * lev : start + count * (lev + 1), :] = value.astype(F32)
    shape = (2 * FR, (TR + 2) * 8)
    lev_of = jnp.where(iota(shape, 0) >= FR, 1, 0)
    inner = iota(shape, 1)
    value = jnp.where((inner & 1) == lev_of, weight(iota(shape, 0) - FR * lev_of, (inner >> 3) - 1), 0)
    prows_w[...] = value.astype(F32).astype(BF16)
    for p in range(3):
        shape = (128, FC)
        at = iota(shape, 0) & 31
        value = jnp.where(at < POS, weight(iota(shape, 1), 3 * at + p - HC), 0)
        pcols_w[128 * p : 128 * (p + 1)] = value.astype(F32).astype(BF16)
        shape = (128, 128)
        at = iota(shape, 1) & 31
        value = jnp.where((at < POS) & (iota(shape, 0) == 32 * p + at), 1, 0)
        spread_w[:, 128 * p : 128 * (p + 1)] = value.astype(F32).astype(BF16)

    def c_copies(app):
        found = []
        for b, col in ((0, west), (1, gy), (2, east)):
            for kind, (row, snd, rcv) in enumerate(((gx, snd_c, rcv_c), (north, snd_n, rcv_n), (south, snd_s, rcv_s))):
                if b == 1 and kind == 0:
                    continue
                found.append(
                    pltpu.make_async_remote_copy(
                        src_ref=snd.at[app, b], dst_ref=rcv.at[app, b],
                        send_sem=c_send.at[app, kind, b], recv_sem=c_recv.at[app, kind, b],
                        device_id=(row, col), device_id_type=MESH,
                    )
                )
        return found

    def restrict(app, v):
        wide = dot_right(v, cols_w[...])
        z = dot_left(rows_w[...].astype(BF16), wide) * NINE
        for b in range(3):
            snd_c[app, b] = z[0:48, 128 * b : 128 * (b + 1)]
            snd_n[app, b] = z[48:80, 128 * b : 128 * (b + 1)]
            snd_s[app, b] = z[80:112, 128 * b : 128 * (b + 1)]

    first = wobs[...] * innov[...]
    vq[0] = first
    restrict(0, first)

    group = iota((24, 128), 1) >> 5
    for odd in range(2):
        shape = (256, 128)
        at = iota(shape, 1)
        from_lane = (128 * (1 - odd) + TC * odd - HC) + 3 * (at & 31) + (at >> 5)
        value = jnp.where(((at & 31) < POS) & (at < 96) & (iota(shape, 0) == from_lane), 1, 0)
        select = value.astype(F32).astype(BF16)
        for j in range(odd, NY, 2):
            lane = 128 * ((j + 1) // 2)
            cut = jnp.dot(raw[:, lane : lane + 256], select, preferred_element_type=F32)
            for row in range(2):
                for p in range(3):
                    x = jnp.zeros((24, 128), F32)
                    for g in range(4):
                        piece = cut[24 * (2 * g + row) : 24 * (2 * g + row + 1)]
                        turn = (32 * (g - p)) % 128
                        x = jnp.where(group == g, pltpu.roll(piece, turn, 1) if turn else piece, x)
                    start = 18 * (3 * row + p)
                    stage[j, start : start + 24] = x
            stage[j, MSG - 4 : MSG] = cut[192:196]
            source[j] = stage[j, 0:MSG].astype(BF16)

    pl.semaphore_wait(barrier, (NY - 1) + (NX - 1) + 4)

    for copy in c_copies(0):
        copy.start()

    moves = []
    for d in range(1, NY):
        col = lax.rem(gy + d, NY)
        moves.append(
            pltpu.make_async_remote_copy(
                src_ref=source.at[col], dst_ref=mbuf.at[gy + 5],
                send_sem=m_send.at[d], recv_sem=m_recv.at[d],
                device_id=(gx, col), device_id_type=MESH,
            )
        )
    for copy in moves:
        copy.start()
    own = pltpu.make_async_copy(source.at[gy], mbuf.at[gy + 5], m_local)
    own.start()

    def halo(side, d):
        g = lax.rem(gy + NY - d, NY)
        return g <= 4 if side == 0 else g >= 3, pltpu.make_async_remote_copy(
            src_ref=source.at[gy] if d == 0 else mbuf.at[g + 5],
            dst_ref=mbuf.at[jnp.minimum(g, 4) + 13 if side == 0 else jnp.maximum(g, 3) - 3],
            send_sem=h_send.at[side, d], recv_sem=h_recv.at[side, d],
            device_id=(north if side == 0 else south, gy), device_id_type=MESH,
        )

    def halo_do(d, what):
        for side in range(2):
            used, copy = halo(side, d)

            @pl.when(used)
            def _():
                getattr(copy, what)()

    halo_do(0, "start")
    for d in range(1, NY):
        moves[d - 1].wait_recv()
        halo_do(d, "start")
    own.wait()

    def unpack(pair):
        unpacked[pair, 0:MSG] = mbuf[pair].astype(F32)
        real = iota((24, 128), 0) < 18
        for row in range(2):
            for p in range(3):
                start = 18 * (3 * row + p)
                x = jnp.where(real, unpacked[pair, start : start + 24], 0.0)
                mf[2 * pair + row, p] = x.reshape(3, 8, 128)
        kcomp[4 * pair : 4 * pair + 4] = unpacked[pair, MSG - 4 : MSG]

    for pair in range(5, 13):
        unpack(pair)
    for d in range(NY):
        halo_do(d, "wait_recv")
    for pair in (0, 1, 2, 3, 4, 13, 14, 15, 16, 17):
        unpack(pair)

    lev_odd = (iota((8, 128), 0) & 1) == 1
    kw[...] = jnp.dot(kcomp[...].astype(BF16), spread_w[...], preferred_element_type=F32)

    def by_level(ref, even, odd, p):
        lanes = slice(128 * p, 128 * (p + 1))
        return jnp.where(
            lev_odd, jnp.broadcast_to(ref[odd : odd + 1, lanes], (8, 128)), jnp.broadcast_to(ref[even : even + 1, lanes], (8, 128))
        )

    on_n, on_s = jnp.where(gx > 0, 1.0, 0.0), jnp.where(gx < NX - 1, 1.0, 0.0)
    for e in range(ER):
        for p in range(3):
            rate = by_level(kw, 2 * e, 2 * e + 1, p)
            rate = rate * (on_n if e < HR else on_s if e >= HR + TR else 1.0)
            known = rate > 0.0
            kbuf[e, p] = rate
            qbuf[e, p] = 1.0 - 4.0 * rate
            ibuf[e, p] = jnp.where(known, 1.0, 0.0)
            rbuf[e, p] = jnp.where(known, 1.0 / jnp.where(known, rate, 1.0) - 4.0, 0.0)

    def apply(app, v):
        for copy in c_copies(app):
            copy.wait_recv()
        mine = snd_c[app, 1] + rcv_c[app, 0] + rcv_c[app, 2]
        north_in = rcv_s[app, 0] + rcv_s[app, 1] + rcv_s[app, 2]
        south_in = rcv_n[app, 0] + rcv_n[app, 1] + rcv_n[app, 2]
        for lev in range(2):
            c, n, s = mine[24 * lev : 24 * lev + 24], north_in[16 * lev : 16 * lev + 16], south_in[16 * lev : 16 * lev + 16]
            cbuf[40 * lev + 0 : 40 * lev + 8] = n[0:8]
            cbuf[40 * lev + 8 : 40 * lev + 16] = n[8:16] + c[0:8]
            cbuf[40 * lev + 16 : 40 * lev + 24] = c[8:16]
            cbuf[40 * lev + 24 : 40 * lev + 32] = c[16:24] + s[0:8]
            cbuf[40 * lev + 32 : 40 * lev + 40] = s[8:16]
        cw[...] = dot_right(cbuf[...], spread_w[...])
        for e in range(1, ER - 1):
            for p in range(3):
                kc[e, p] = by_level(cw, e, 40 + e, p) * kbuf[e, p]
        bufs = (xa, xb)
        for t in range(2 * NPASS):
            src, dst = bufs[t % 2], bufs[(t + 1) % 2]

            def row(r, src=src, t=t):
                return [mf[r, p] * kc[r, p][None] if t == 0 else src[r, p] for p in range(3)]

            def store(r, p, x, dst=dst, t=t):
                if t == 2 * NPASS - 1:
                    at = 8 * (r - HR + 1)
                    acc[at : at + 8, 128 * p : 128 * (p + 1)] = jnp.sum(x * mf[r, p], axis=0)
                else:
                    dst[r, p] = x

            middle = t == NPASS - 1
            diffuse(row, store, rbuf if middle else qbuf, ibuf if middle else kbuf, 2 + t, ER - 2 - t)
        tall = dot_left(prows_w[...], acc[...])
        scale = sscale[...]
        return scale * scale * v + dot_right(tall, pcols_w[...]) * NINE

    lane = iota((1, 128), 1)

    def pack(pairs):
        out = jnp.zeros((1, 128), F32)
        for i, (left, right) in enumerate(pairs):
            total = jnp.sum(jnp.sum(left * right, axis=0, keepdims=True), axis=1, keepdims=True)
            out = jnp.where(lane == i, total, out)
        return out

    def y_copy(use, d):
        return pltpu.make_async_remote_copy(
            src_ref=red_own.at[use], dst_ref=red_y.at[use, d], send_sem=ry_send.at[use, d], recv_sem=ry_recv.at[use, d],
            device_id=(gx, lax.rem(gy + d, NY)), device_id_type=MESH,
        )

    def x_copy(use, d):
        return pltpu.make_async_remote_copy(
            src_ref=red_own2.at[use], dst_ref=red_x.at[use, d], send_sem=rx_send.at[use, d], recv_sem=rx_recv.at[use, d],
            device_id=(lax.rem(gx + d, NX), gy), device_id_type=MESH,
        )

    def each(count, make, what):
        def body(d, _):
            getattr(make(d), what)()
            return 0

        lax.fori_loop(1, count, body, 0)

    def reduce_start(use, row):
        red_own[use] = row
        each(NY, functools.partial(y_copy, use), "start")

    def reduce_middle(use):
        each(NY, functools.partial(y_copy, use), "wait_recv")
        total = red_own[use]
        for d in range(1, NY):
            total = total + red_y[use, d]
        red_own2[use] = total
        each(NX, functools.partial(x_copy, use), "start")

    def reduce_end(use):
        each(NX, functools.partial(x_copy, use), "wait_recv")
        total = red_own2[use]
        for d in range(1, NX):
            total = total + red_x[use, d]
        each(NY, functools.partial(y_copy, use), "wait_send")
        each(NX, functools.partial(x_copy, use), "wait_send")
        return total

    def pick(row, i):
        return jnp.sum(jnp.where(lane == i, row, 0.0), axis=1, keepdims=True)

    w = wobs[...]
    b0 = apply(0, vq[0])
    vb[0] = b0
    q1 = w * b0
    restrict(1, q1)
    for copy in c_copies(1):
        copy.start()
    reduce_start(0, pack(((vq[0], b0), (q1, b0))))
    vq[1] = q1
    reduce_middle(0)
    b1 = apply(1, vq[1])
    sums = reduce_end(0)
    theta = pick(sums, 1) / pick(sums, 0)
    b1 = b1 - theta * vb[0]
    vq[1] = vq[1] - theta * vq[0]
    vb[1] = b1
    q2 = w * b1
    restrict(2, q2)
    for copy in c_copies(2):
        copy.start()
    vq[2] = q2
    b2 = apply(2, vq[2])
    vb[2] = b2
    q0, q1, b0, b1 = vq[0], vq[1], vb[0], vb[1]
    wb = (w * b0, w * b1, w * b2)
    q2 = vq[2]
    row = pack((
        (q0, b0), (q0, b1), (q0, b2), (q1, b1), (q1, b2), (q2, b2),
        (b0, wb[0]), (b0, wb[1]), (b0, wb[2]), (b1, wb[1]), (b1, wb[2]), (b2, wb[2]),
    ))
    reduce_start(1, row)
    reduce_middle(1)
    sums = reduce_end(1)
    e = [pick(sums, i) for i in range(12)]
    s00, s01, s02, s11, s12, s22 = [e[i] + e[6 + i] for i in range(6)]
    tiny = 1e-7
    i0 = 1.0 / s00
    l10, l20 = s01 * i0, s02 * i0
    d1 = s11 - l10 * s01
    i1 = jnp.where(d1 > tiny * s11, 1.0 / d1, 0.0)
    t12 = s12 - l10 * s02
    l21 = t12 * i1
    d2 = s22 - l20 * s02 - l21 * t12
    i2 = jnp.where(d2 > tiny * s22, 1.0 / d2, 0.0)
    r0, r1, r2 = e[0], e[1], e[2]
    r1 = r1 - l10 * r0
    r2 = r2 - l20 * r0 - l21 * r1
    z2 = r2 * i2
    z1 = r1 * i1 - l21 * z2
    z0 = r0 * i0 - l10 * z1 - l20 * z2
    inc_ref[...] = z0 * vb[0] + z1 * vb[1] + z2 * vb[2]
    stat_ref[...] = sscale[...] * (z0 * vq[0] + z1 * vq[1] + z2 * vq[2])

    for app in range(3):
        for copy in c_copies(app):
            copy.wait_send()
    for copy in moves:
        copy.wait_send()
    for d in range(NY):
        halo_do(d, "wait_send")


def per_device(NX, NY, innovation, obs_weight, static_scale, members, diffusivity):
    wide = members.shape[-1]
    m = members.reshape(4, 9, 2, 2, wide).transpose(0, 3, 1, 2, 4).reshape(8, 18, wide)
    m = jnp.pad(m, ((0, 0), (0, 6), (0, 0))).reshape(192, wide)
    k = jnp.pad(diffusivity.transpose(1, 0, 2).reshape(4, wide), ((0, 12), (0, 0)))
    raw = jnp.pad(jnp.concatenate([m, k]), ((0, 0), (128, 128)))
    vec = (2 * FR, FC)
    vmem = pl.BlockSpec(memory_space=pltpu.VMEM)
    dma = pltpu.SemaphoreType.DMA
    inc, stat = pl.pallas_call(
        functools.partial(kernel, NX, NY),
        out_shape=(jax.ShapeDtypeStruct(vec, F32), jax.ShapeDtypeStruct(vec, F32)),
        in_specs=[vmem] * 4,
        out_specs=(vmem, vmem),
        scratch_shapes=[
            pltpu.VMEM((PAIRS, MSG, 128), BF16),
            pltpu.VMEM((ER, 3, 3, 8, 128), F32),
            pltpu.VMEM((ER, 3, 3, 8, 128), F32),
            pltpu.VMEM((ER, 3, 3, 8, 128), F32),
            pltpu.VMEM((ER, 3, 8, 128), F32),
            pltpu.VMEM((ER, 3, 8, 128), F32),
            pltpu.VMEM((ER, 3, 8, 128), F32),
            pltpu.VMEM((ER, 3, 8, 128), F32),
            pltpu.VMEM((ER, 3, 8, 128), F32),
            pltpu.VMEM(((TR + 2) * 8, 384), F32),
            pltpu.VMEM((80, 128), F32),
            pltpu.VMEM((80, 384), F32),
            pltpu.VMEM((2 * ER, 384), F32),
            pltpu.VMEM((2 * ER, 128), F32),
            pltpu.VMEM((NY, MSG + 8, 128), F32),
            pltpu.VMEM((NY, MSG, 128), BF16),
            pltpu.VMEM((PAIRS, MSG + 8, 128), F32),
            pltpu.VMEM((112, 2 * FR), F32),
            pltpu.VMEM((FC, 384), BF16),
            pltpu.VMEM((2 * FR, (TR + 2) * 8), BF16),
            pltpu.VMEM((384, FC), BF16),
            pltpu.VMEM((128, 384), BF16),
            pltpu.VMEM((3, 3, 48, 128), F32),
            pltpu.VMEM((3, 3, 32, 128), F32),
            pltpu.VMEM((3, 3, 32, 128), F32),
            pltpu.VMEM((3, 3, 48, 128), F32),
            pltpu.VMEM((3, 3, 32, 128), F32),
            pltpu.VMEM((3, 3, 32, 128), F32),
            pltpu.VMEM((3,) + vec, F32),
            pltpu.VMEM((3,) + vec, F32),
            pltpu.VMEM((2, 1, 128), F32),
            pltpu.VMEM((2, NY, 1, 128), F32),
            pltpu.VMEM((2, 1, 128), F32),
            pltpu.VMEM((2, NX, 1, 128), F32),
            dma((NY,)), dma((NY,)), dma,
            dma((2, NY)), dma((2, NY)),
            dma((3, 3, 3)), dma((3, 3, 3)),
            dma((2, NY)), dma((2, NY)),
            dma((2, NX)), dma((2, NX)),
        ],
        compiler_params=pltpu.CompilerParams(collective_id=0, has_side_effects=True),
        name="solve",
    )(innovation.reshape(vec), obs_weight.reshape(vec), static_scale.reshape(vec), raw)
    return inc.reshape(2, FR, FC), stat.reshape(2, FR, FC)


def solution(mesh):
    NX, NY = mesh.shape["gx"], mesh.shape["gy"]
    fine = P(None, "gx", "gy")
    return jax.shard_map(
        functools.partial(per_device, NX, NY),
        mesh=mesh,
        in_specs=(fine, fine, fine, P(None, None, ("gx", "gy"), None), P(None, ("gx", "gy"), None)),
        out_specs=(fine, fine),
        check_vma=False,
    )
```

```python
import functools

import jax
import jax.numpy as jnp
from jax import lax
from jax.experimental import pallas as pl
from jax.experimental.pallas import tpu as pltpu
from jax.sharding import PartitionSpec as P

TR, TC, FR, FC = 16, 64, 48, 192
HR, HC, ER, POS = 10, 9, 36, 28
MSG = 112
PAIRS = ER // 2
NPASS = 4
F32, BF16 = jnp.float32, jnp.bfloat16
MESH = pl.DeviceIdType.MESH
NINE = 1.0 / 9.0


def iota(shape, dim):
    return lax.broadcasted_iota(jnp.int32, shape, dim)


def weight(fine, coarse):
    return jnp.maximum(3 - jnp.abs(fine - 3 * coarse - 1), 0)


def parts(x):
    high = x.astype(BF16)
    rest = x - high.astype(F32)
    mid = rest.astype(BF16)
    low = (rest - mid.astype(F32)).astype(BF16)
    return high, mid, low


def dot_left(const, x):
    return functools.reduce(jnp.add, [jnp.dot(const, p, preferred_element_type=F32) for p in parts(x)])


def dot_right(x, const):
    return functools.reduce(jnp.add, [jnp.dot(p, const, preferred_element_type=F32) for p in parts(x)])


def diffuse(row, store, center, around, first, last):
    above, here = row(first - 1), row(first)
    for r in range(first, last):
        below = row(r + 1)
        for p in range(3):
            before = here[p - 1] if p else pltpu.roll(here[2], 1, 2)
            after = here[p + 1] if p < 2 else pltpu.roll(here[0], 127, 2)
            near = (above[p] + below[p]) + (before + after)
            store(r, p, center[r, p][None] * here[p] + around[r, p][None] * near)
        above, here = here, below


def kernel(
    NX, NY, innov_in, wobs_in, sscale_in, members_in, rates_in,
    inc_ref, stat_ref,
    innov, wobs, sscale, members, rates, raw,
    mbuf, mf, xa, xb, kbuf, qbuf, ibuf, rbuf, kc, acc, cbuf, cw, kw, kcomp, stage, source, unpacked,
    rows_w, cols_w, prows_w, pcols_w, spread_w,
    snd_c, snd_n, snd_s, snd_side, rcv_n, rcv_s, rcv_side,
    vq, vb, last, red_own, red_y, red_own2, red_x,
    in_sem, m_send, m_recv, m_local, h_send, h_recv, c_send, c_recv, ry_send, ry_recv, rx_send, rx_recv,
):
    gx, gy = lax.axis_index("gx"), lax.axis_index("gy")
    north, south = lax.rem(gx + NX - 1, NX), lax.rem(gx + 1, NX)
    west, east = lax.rem(gy + NY - 1, NY), lax.rem(gy + 1, NY)

    barrier = pltpu.get_barrier_semaphore()
    for d in sorted(range(1, NX), key=lambda d: min(d % 8, 8 - d % 8), reverse=True):
        pl.semaphore_signal(barrier, inc=1, device_id=(lax.rem(gx + d, NX), gy), device_id_type=MESH)
    for row in (north, south):
        for col in (west, east):
            pl.semaphore_signal(barrier, inc=1, device_id=(row, col), device_id_type=MESH)
    for d in range(1, NY):
        pl.semaphore_signal(barrier, inc=1, device_id=(gx, lax.rem(gy + d, NY)), device_id_type=MESH)

    loads = [
        pltpu.make_async_copy(src, dst, in_sem.at[i])
        for i, (src, dst) in enumerate(
            ((innov_in, innov), (wobs_in, wobs), (sscale_in, sscale), (members_in, members), (rates_in, rates))
        )
    ]
    for copy in loads:
        copy.start()

    has_n = jnp.where(gx > 0, 1, 0)
    has_s = jnp.where(gx < NX - 1, 1, 0)
    has_w = jnp.where(gy > 0, 1, 0)
    has_e = jnp.where(gy < NY - 1, 1, 0)
    for b, on in ((0, has_w), (1, 1), (2, has_e)):
        shape = (FC, 128)
        at = iota(shape, 1)
        cell = 3 * (at & 31) + (at >> 5) - HC + TC * (b - 1)
        value = jnp.where(((at & 31) < POS) & (at < 96), weight(iota(shape, 0), cell) * on, 0)
        cols_w[:, 128 * b : 128 * (b + 1)] = value.astype(F32).astype(BF16)
    for start, count, shift, on in ((0, 24, -2, 1), (48, 16, -2, has_n), (80, 16, 6, has_s)):
        shape = (count, 2 * FR)
        for lev in range(2):
            fine = iota(shape, 1) - FR * lev
            value = jnp.where((fine >= 0) & (fine < FR), weight(fine, iota(shape, 0) + shift) * on, 0)
            rows_w[start + count * lev : start + count * (lev + 1), :] = value.astype(F32)
    place = iota((8, 128), 1) & 31

    def squeeze(x, side):
        out = jnp.zeros((8, 128), F32)
        for i in range(x.shape[0] // 8):
            turn = (4 * i - (0 if side == 2 else POS - 4)) % 128
            block = x[8 * i : 8 * i + 8]
            out = jnp.where((place >> 2) == i, pltpu.roll(block, turn, 1) if turn else block, out)
        return out

    def spread_out(x, count, side):
        base = 0 if side == 2 else POS - 4
        out = []
        for i in range(count):
            turn = (base - 4 * i) % 128
            out.append(jnp.where((place >> 2) == base // 4, pltpu.roll(x, turn, 1) if turn else x, 0.0))
        return jnp.concatenate(out)

    def c_copies(app):
        found = []
        for b, col in ((0, west), (2, east), (1, gy)):
            for kind, (row, snd, rcv) in enumerate(((gx, snd_c, snd_c), (north, snd_n, rcv_n), (south, snd_s, rcv_s))):
                if b == 1 and kind == 0:
                    continue
                found.append(
                    pltpu.make_async_remote_copy(
                        src_ref=snd.at[app] if b == 1 else snd_side.at[app, kind, b // 2],
                        dst_ref=rcv.at[app] if b == 1 else rcv_side.at[app, kind, b // 2],
                        send_sem=c_send.at[app, kind, b], recv_sem=c_recv.at[app, kind, b],
                        device_id=(row, col), device_id_type=MESH,
                    )
                )
        return found

    def restrict(app, v):
        wide = dot_right(v, cols_w[...])
        z = dot_left(rows_w[...].astype(BF16), wide) * NINE
        for kind, (start, count, ref) in enumerate(((0, 48, snd_c), (48, 32, snd_n), (80, 32, snd_s))):
            for b in (0, 2):
                snd_side[app, kind, b // 2] = squeeze(z[start : start + count, 128 * b : 128 * (b + 1)], b)
            ref[app] = z[start : start + count, 128:256]

    loads[0].wait()
    loads[1].wait()
    first = wobs[...] * innov[...]
    vq[0] = first
    restrict(0, first)

    loads[3].wait()
    loads[4].wait()
    wide = members.shape[-1]
    natural = members[...].astype(F32).reshape(144, wide).astype(BF16)
    shape = (24, 144)
    at = iota(shape, 0)
    zero = jnp.zeros((208, 128), BF16)
    raw[:, 0:128] = zero
    raw[:, 128 + wide : 256 + wide] = zero
    order = []
    for g in range(4):
        for row in range(2):
            value = jnp.where((at < 18) & (iota(shape, 1) == (9 * g + (at >> 1)) * 4 + (at & 1) * 2 + row), 1, 0)
            order.append(value.astype(F32).astype(BF16))
    raw[0:192, 128 : 128 + wide] = jnp.dot(
        jnp.concatenate(order), natural, preferred_element_type=F32
    ).astype(BF16)
    by_lev = rates[...].astype(F32).reshape(4, wide)
    kcomp[0:16] = jnp.zeros((16, 128), F32)
    for tile in range(wide // 128):
        lanes = slice(128 * tile, 128 * (tile + 1))
        for at_row, of in enumerate((0, 2, 1, 3)):
            kcomp[at_row : at_row + 1] = by_lev[of : of + 1, lanes]
        raw[192:208, 128 + 128 * tile : 256 + 128 * tile] = kcomp[0:16].astype(BF16)
    group = iota((24, 128), 1) >> 5
    for odd in range(2):
        shape = (256, 128)
        at = iota(shape, 1)
        from_lane = (128 * (1 - odd) + TC * odd - HC) + 3 * (at & 31) + (at >> 5)
        value = jnp.where(((at & 31) < POS) & (at < 96) & (iota(shape, 0) == from_lane), 1, 0)
        select = value.astype(F32).astype(BF16)
        for j in range(odd, NY, 2):
            lane = 128 * ((j + 1) // 2)
            cut = jnp.dot(raw[:, lane : lane + 256], select, preferred_element_type=F32)
            for row in range(2):
                for p in range(3):
                    x = jnp.zeros((24, 128), F32)
                    for g in range(4):
                        piece = cut[24 * (2 * g + row) : 24 * (2 * g + row + 1)]
                        turn = (32 * (g - p)) % 128
                        x = jnp.where(group == g, pltpu.roll(piece, turn, 1) if turn else piece, x)
                    start = 18 * (3 * row + p)
                    stage[j, start : start + 24] = x
            stage[j, MSG - 4 : MSG] = cut[192:196]
            source[j] = stage[j, 0:MSG].astype(BF16)

    pl.semaphore_wait(barrier, (NY - 1) + (NX - 1) + 4)

    for copy in c_copies(0):
        copy.start()

    moves = []
    for d in range(1, NY):
        col = lax.rem(gy + d, NY)
        moves.append(
            pltpu.make_async_remote_copy(
                src_ref=source.at[col], dst_ref=mbuf.at[gy + 5],
                send_sem=m_send.at[d], recv_sem=m_recv.at[d],
                device_id=(gx, col), device_id_type=MESH,
            )
        )
    for copy in moves:
        copy.start()
    own = pltpu.make_async_copy(source.at[gy], mbuf.at[gy + 5], m_local)
    own.start()

    shape = (2 * FR, (TR + 2) * 8)
    lev_of = jnp.where(iota(shape, 0) >= FR, 1, 0)
    inner = iota(shape, 1)
    value = jnp.where((inner & 1) == lev_of, weight(iota(shape, 0) - FR * lev_of, (inner >> 3) - 1), 0)
    prows_w[...] = value.astype(F32).astype(BF16)
    for p in range(3):
        shape = (128, FC)
        at = iota(shape, 0) & 31
        value = jnp.where(at < POS, weight(iota(shape, 1), 3 * at + p - HC), 0)
        pcols_w[128 * p : 128 * (p + 1)] = value.astype(F32).astype(BF16)
        shape = (128, 128)
        at = iota(shape, 1) & 31
        value = jnp.where((at < POS) & (iota(shape, 0) == 32 * p + at), 1, 0)
        spread_w[:, 128 * p : 128 * (p + 1)] = value.astype(F32).astype(BF16)

    def halo(side, d):
        g = lax.rem(gy + NY - d, NY)
        return g <= 4 if side == 0 else g >= 3, pltpu.make_async_remote_copy(
            src_ref=source.at[gy] if d == 0 else mbuf.at[g + 5],
            dst_ref=mbuf.at[jnp.minimum(g, 4) + 13 if side == 0 else jnp.maximum(g, 3) - 3],
            send_sem=h_send.at[side, d], recv_sem=h_recv.at[side, d],
            device_id=(north if side == 0 else south, gy), device_id_type=MESH,
        )

    def halo_do(d, what):
        for side in range(2):
            used, copy = halo(side, d)

            @pl.when(used)
            def _():
                getattr(copy, what)()

    halo_do(0, "start")
    for d in range(1, NY):
        moves[d - 1].wait_recv()
        halo_do(d, "start")
    own.wait()

    def unpack(pair):
        unpacked[pair, 0:MSG] = mbuf[pair].astype(F32)
        real = iota((24, 128), 0) < 18
        for row in range(2):
            for p in range(3):
                start = 18 * (3 * row + p)
                x = jnp.where(real, unpacked[pair, start : start + 24], 0.0)
                mf[2 * pair + row, p] = x.reshape(3, 8, 128)
        kcomp[4 * pair : 4 * pair + 4] = unpacked[pair, MSG - 4 : MSG]

    loads[2].wait()
    for pair in range(5, 13):
        unpack(pair)
    for d in range(NY):
        halo_do(d, "wait_recv")
    for pair in (0, 1, 2, 3, 4, 13, 14, 15, 16, 17):
        unpack(pair)

    lev_odd = (iota((8, 128), 0) & 1) == 1
    kw[...] = jnp.dot(kcomp[...].astype(BF16), spread_w[...], preferred_element_type=F32)

    def by_level(ref, even, odd, p):
        lanes = slice(128 * p, 128 * (p + 1))
        return jnp.where(
            lev_odd, jnp.broadcast_to(ref[odd : odd + 1, lanes], (8, 128)), jnp.broadcast_to(ref[even : even + 1, lanes], (8, 128))
        )

    on_n, on_s = jnp.where(gx > 0, 1.0, 0.0), jnp.where(gx < NX - 1, 1.0, 0.0)
    for e in range(ER):
        for p in range(3):
            rate = by_level(kw, 2 * e, 2 * e + 1, p)
            rate = rate * (on_n if e < HR else on_s if e >= HR + TR else 1.0)
            known = rate > 0.0
            kbuf[e, p] = rate
            qbuf[e, p] = 1.0 - 4.0 * rate
            ibuf[e, p] = jnp.where(known, 1.0, 0.0)
            rbuf[e, p] = jnp.where(known, 1.0 / jnp.where(known, rate, 1.0) - 4.0, 0.0)

    def apply(app, v):
        for copy in c_copies(app):
            copy.wait_recv()
        def total(kind, middle):
            count = middle.shape[0] // 8
            sides = [spread_out(rcv_side[app, kind, b // 2], count, b) for b in (0, 2)]
            return middle + (sides[0] + sides[1])

        mine = total(0, snd_c[app])
        north_in = total(2, rcv_s[app])
        south_in = total(1, rcv_n[app])
        for lev in range(2):
            c, n, s = mine[24 * lev : 24 * lev + 24], north_in[16 * lev : 16 * lev + 16], south_in[16 * lev : 16 * lev + 16]
            cbuf[40 * lev + 0 : 40 * lev + 8] = n[0:8]
            cbuf[40 * lev + 8 : 40 * lev + 16] = n[8:16] + c[0:8]
            cbuf[40 * lev + 16 : 40 * lev + 24] = c[8:16]
            cbuf[40 * lev + 24 : 40 * lev + 32] = c[16:24] + s[0:8]
            cbuf[40 * lev + 32 : 40 * lev + 40] = s[8:16]
        cw[...] = dot_right(cbuf[...], spread_w[...])
        for e in range(1, ER - 1):
            for p in range(3):
                kc[e, p] = by_level(cw, e, 40 + e, p) * kbuf[e, p]
        bufs = (xa, xb)
        for t in range(2 * NPASS):
            src, dst = bufs[t % 2], bufs[(t + 1) % 2]

            def row(r, src=src, t=t):
                return [mf[r, p] * kc[r, p][None] if t == 0 else src[r, p] for p in range(3)]

            def store(r, p, x, dst=dst, t=t):
                if t == 2 * NPASS - 1:
                    at = 8 * (r - HR + 1)
                    acc[at : at + 8, 128 * p : 128 * (p + 1)] = jnp.sum(x * mf[r, p], axis=0)
                else:
                    dst[r, p] = x

            middle = t == NPASS - 1
            diffuse(row, store, rbuf if middle else qbuf, ibuf if middle else kbuf, 2 + t, ER - 2 - t)
        tall = dot_left(prows_w[...], acc[...])
        scale = sscale[...]
        return scale * scale * v + dot_right(tall, pcols_w[...]) * NINE

    lane = iota((1, 128), 1)

    def pack(pairs, first=0):
        out = jnp.zeros((1, 128), F32)
        for i, (left, right) in enumerate(pairs):
            total = jnp.sum(jnp.sum(left * right, axis=0, keepdims=True), axis=1, keepdims=True)
            out = jnp.where(lane == i + first, total, out)
        return out

    def y_copy(use, d):
        return pltpu.make_async_remote_copy(
            src_ref=red_own.at[use], dst_ref=red_y.at[use, d], send_sem=ry_send.at[use, d], recv_sem=ry_recv.at[use, d],
            device_id=(gx, lax.rem(gy + d, NY)), device_id_type=MESH,
        )

    def x_copy(use, d):
        return pltpu.make_async_remote_copy(
            src_ref=red_own2.at[use], dst_ref=red_x.at[use, d], send_sem=rx_send.at[use, d], recv_sem=rx_recv.at[use, d],
            device_id=(lax.rem(gx + d, NX), gy), device_id_type=MESH,
        )

    def each(count, make, what):
        def body(d, _):
            getattr(make(d), what)()
            return 0

        lax.fori_loop(1, count, body, 0)

    def reduce_start(use, row):
        red_own[use] = row
        each(NY, functools.partial(y_copy, use), "start")

    def reduce_middle(use):
        each(NY, functools.partial(y_copy, use), "wait_recv")
        total = red_own[use]
        for d in range(1, NY):
            total = total + red_y[use, d]
        red_own2[use] = total
        each(NX, functools.partial(x_copy, use), "start")

    def reduce_end(use):
        each(NX, functools.partial(x_copy, use), "wait_recv")
        total = red_own2[use]
        for d in range(1, NX):
            total = total + red_x[use, d]
        each(NY, functools.partial(y_copy, use), "wait_send")
        each(NX, functools.partial(x_copy, use), "wait_send")
        return total

    def pick(row, i):
        return jnp.sum(jnp.where(lane == i, row, 0.0), axis=1, keepdims=True)

    w = wobs[...]
    b0 = apply(0, vq[0])
    vb[0] = b0
    q1 = w * b0
    restrict(1, q1)
    for copy in c_copies(1):
        copy.start()
    reduce_start(0, pack(((vq[0], b0), (q1, b0))))
    vq[1] = q1
    reduce_middle(0)
    b1 = apply(1, vq[1])
    q2 = w * b1
    restrict(2, q2)
    for copy in c_copies(2):
        copy.start()
    vq[2] = q2
    sums = reduce_end(0)
    theta = pick(sums, 1) / pick(sums, 0)
    last[1] = theta * b1
    q0, b0 = vq[0], vb[0]
    q2 = q2 - theta * vq[1]
    last[0] = q2
    q1 = vq[1] - theta * q0
    vq[1] = q1
    b1 = b1 - theta * b0
    vb[1] = b1
    early = pack(((q0, b0), (q0, b1), (b0, q2), (q1, b1), (b1, q2), (b0, w * b0), (b0, w * b1), (b1, w * b1)))
    b2 = apply(2, vq[2]) - last[1]
    vb[2] = b2
    vq[2] = last[0]
    late = pack(((vq[2], b2), (b2, wobs[...] * b2)), 8)
    row = jnp.where(lane >= 8, late, early)
    reduce_start(1, row)
    reduce_middle(1)
    sums = reduce_end(1)
    e00, e01, e02, e11, e12, f00, f01, f11, e22, f22 = [pick(sums, i) for i in range(10)]
    s00, s01, s02 = e00 + f00, e01 + f01, e02 + (e12 + theta * e02)
    s11, s12, s22 = e11 + f11, e12 + e22, e22 + f22
    tiny = 1e-7
    i0 = 1.0 / s00
    l10, l20 = s01 * i0, s02 * i0
    d1 = s11 - l10 * s01
    i1 = jnp.where(d1 > tiny * s11, 1.0 / d1, 0.0)
    t12 = s12 - l10 * s02
    l21 = t12 * i1
    d2 = s22 - l20 * s02 - l21 * t12
    i2 = jnp.where(d2 > tiny * s22, 1.0 / d2, 0.0)
    r0, r1, r2 = e00, e01, e02
    r1 = r1 - l10 * r0
    r2 = r2 - l20 * r0 - l21 * r1
    z2 = r2 * i2
    z1 = r1 * i1 - l21 * z2
    z0 = r0 * i0 - l10 * z1 - l20 * z2
    inc_ref[...] = z0 * vb[0] + z1 * vb[1] + z2 * vb[2]
    stat_ref[...] = sscale[...] * (z0 * vq[0] + z1 * vq[1] + z2 * vq[2])

    for app in range(3):
        for copy in c_copies(app):
            copy.wait_send()
    for copy in moves:
        copy.wait_send()
    for d in range(NY):
        halo_do(d, "wait_send")


def per_device(NX, NY, innovation, obs_weight, static_scale, members, diffusivity):
    vec = (2 * FR, FC)
    vmem = pl.BlockSpec(memory_space=pltpu.VMEM)
    dma = pltpu.SemaphoreType.DMA
    inc, stat = pl.pallas_call(
        functools.partial(kernel, NX, NY),
        out_shape=(jax.ShapeDtypeStruct(vec, F32), jax.ShapeDtypeStruct(vec, F32)),
        in_specs=[pl.BlockSpec(memory_space=pl.ANY)] * 5,
        out_specs=(vmem, vmem),
        scratch_shapes=[
            pltpu.VMEM(vec, F32),
            pltpu.VMEM(vec, F32),
            pltpu.VMEM(vec, F32),
            pltpu.VMEM(members.shape, BF16),
            pltpu.VMEM(diffusivity.shape, BF16),
            pltpu.VMEM((208, members.shape[-1] + 256), BF16),
            pltpu.VMEM((PAIRS, MSG, 128), BF16),
            pltpu.VMEM((ER, 3, 3, 8, 128), F32),
            pltpu.VMEM((ER, 3, 3, 8, 128), F32),
            pltpu.VMEM((ER, 3, 3, 8, 128), F32),
            pltpu.VMEM((ER, 3, 8, 128), F32),
            pltpu.VMEM((ER, 3, 8, 128), F32),
            pltpu.VMEM((ER, 3, 8, 128), F32),
            pltpu.VMEM((ER, 3, 8, 128), F32),
            pltpu.VMEM((ER, 3, 8, 128), F32),
            pltpu.VMEM(((TR + 2) * 8, 384), F32),
            pltpu.VMEM((80, 128), F32),
            pltpu.VMEM((80, 384), F32),
            pltpu.VMEM((2 * ER, 384), F32),
            pltpu.VMEM((2 * ER, 128), F32),
            pltpu.VMEM((NY, MSG + 8, 128), F32),
            pltpu.VMEM((NY, MSG, 128), BF16),
            pltpu.VMEM((PAIRS, MSG + 8, 128), F32),
            pltpu.VMEM((112, 2 * FR), F32),
            pltpu.VMEM((FC, 384), BF16),
            pltpu.VMEM((2 * FR, (TR + 2) * 8), BF16),
            pltpu.VMEM((384, FC), BF16),
            pltpu.VMEM((128, 384), BF16),
            pltpu.VMEM((3, 48, 128), F32),
            pltpu.VMEM((3, 32, 128), F32),
            pltpu.VMEM((3, 32, 128), F32),
            pltpu.VMEM((3, 3, 2, 8, 128), F32),
            pltpu.VMEM((3, 32, 128), F32),
            pltpu.VMEM((3, 32, 128), F32),
            pltpu.VMEM((3, 3, 2, 8, 128), F32),
            pltpu.VMEM((3,) + vec, F32),
            pltpu.VMEM((3,) + vec, F32),
            pltpu.VMEM((2,) + vec, F32),
            pltpu.VMEM((2, 1, 128), F32),
            pltpu.VMEM((2, NY, 1, 128), F32),
            pltpu.VMEM((2, 1, 128), F32),
            pltpu.VMEM((2, NX, 1, 128), F32),
            dma((5,)), dma((NY,)), dma((NY,)), dma,
            dma((2, NY)), dma((2, NY)),
            dma((3, 3, 3)), dma((3, 3, 3)),
            dma((2, NY)), dma((2, NY)),
            dma((2, NX)), dma((2, NX)),
        ],
        compiler_params=pltpu.CompilerParams(collective_id=0, has_side_effects=True),
        name="solve",
    )(innovation.reshape(vec), obs_weight.reshape(vec), static_scale.reshape(vec), members, diffusivity)
    return inc.reshape(2, FR, FC), stat.reshape(2, FR, FC)


def solution(mesh):
    NX, NY = mesh.shape["gx"], mesh.shape["gy"]
    fine = P(None, "gx", "gy")
    return jax.shard_map(
        functools.partial(per_device, NX, NY),
        mesh=mesh,
        in_specs=(fine, fine, fine, P(None, None, ("gx", "gy"), None), P(None, ("gx", "gy"), None)),
        out_specs=(fine, fine),
        check_vma=False,
    )
```

```python
import functools

import jax
import jax.numpy as jnp
from jax import lax
from jax.experimental import pallas as pl
from jax.experimental.pallas import tpu as pltpu
from jax.sharding import PartitionSpec as P

TR, TC, FR, FC = 16, 64, 48, 192
HR, HC, ER, POS = 10, 9, 36, 28
MSG = 112
PAIRS = ER // 2
NPASS = 4
F32, BF16 = jnp.float32, jnp.bfloat16
MESH = pl.DeviceIdType.MESH
NINE = 1.0 / 9.0


def iota(shape, dim):
    return lax.broadcasted_iota(jnp.int32, shape, dim)


def weight(fine, coarse):
    return jnp.maximum(3 - jnp.abs(fine - 3 * coarse - 1), 0)


def parts(x):
    high = x.astype(BF16)
    return high, (x - high.astype(F32)).astype(BF16)


def dot_left(const, x):
    return functools.reduce(jnp.add, [jnp.dot(const, p, preferred_element_type=F32) for p in parts(x)])


def dot_right(x, const):
    return functools.reduce(jnp.add, [jnp.dot(p, const, preferred_element_type=F32) for p in parts(x)])


def diffuse(row, store, center, around, first, last):
    above, here = row(first - 1), row(first)
    for r in range(first, last):
        below = row(r + 1)
        for p in range(3):
            before = here[p - 1] if p else pltpu.roll(here[2], 1, 2)
            after = here[p + 1] if p < 2 else pltpu.roll(here[0], 127, 2)
            near = (above[p] + below[p]) + (before + after)
            store(r, p, center[r, p][None] * here[p] + around[r, p][None] * near)
        above, here = here, below


def kernel(
    NX, NY, innov_in, wobs_in, sscale_in, members_in, rates_in,
    inc_ref, stat_ref,
    innov, wobs, sscale, members, rates, raw,
    mbuf, mf, xa, xb, kbuf, qbuf, ibuf, rbuf, kc, acc, cbuf, cw, kw, kcomp, stage, source, unpacked,
    rows_w, cols_w, prows_w, pcols_w, spread_w,
    snd_c, snd_n, snd_s, snd_side, rcv_n, rcv_s, rcv_side,
    vq, vb, last, red_own, red_y, red_own2, red_x,
    in_sem, m_send, m_recv, m_local, h_send, h_recv, c_send, c_recv, ry_send, ry_recv, rx_send, rx_recv,
):
    gx, gy = lax.axis_index("gx"), lax.axis_index("gy")
    north, south = lax.rem(gx + NX - 1, NX), lax.rem(gx + 1, NX)
    west, east = lax.rem(gy + NY - 1, NY), lax.rem(gy + 1, NY)

    barrier = pltpu.get_barrier_semaphore()

    def along_z(d):
        z = lax.rem(2 * lax.div(gx, 8) + lax.rem(gy, 2) + d, NX // 4)
        return 8 * lax.div(z, 2) + lax.rem(gx, 8), 2 * lax.div(gy, 2) + lax.rem(z, 2)

    def in_plane(d):
        u = lax.rem(4 * lax.rem(gx, 8) + lax.div(gy, 2) + d, 4 * NY)
        return 8 * lax.div(gx, 8) + lax.div(u, 4), 2 * lax.rem(u, 4) + lax.rem(gy, 2)

    for d in range(1, NX // 4):
        pl.semaphore_signal(barrier, inc=1, device_id=along_z(d), device_id_type=MESH)
    for d in range(1, 4 * NY):
        pl.semaphore_signal(barrier, inc=1, device_id=in_plane(d), device_id_type=MESH)
    for row in (north, south):
        for col in (west, gy, east):
            pl.semaphore_signal(barrier, inc=1, device_id=(row, col), device_id_type=MESH)
    for d in range(1, NY):
        pl.semaphore_signal(barrier, inc=1, device_id=(gx, lax.rem(gy + d, NY)), device_id_type=MESH)

    loads = [
        pltpu.make_async_copy(src, dst, in_sem.at[i])
        for i, (src, dst) in enumerate(
            ((innov_in, innov), (wobs_in, wobs), (sscale_in, sscale), (members_in, members), (rates_in, rates))
        )
    ]
    for copy in loads:
        copy.start()

    place = iota((8, 128), 1) & 31

    def squeeze(x, side):
        out = jnp.zeros((8, 128), F32)
        for i in range(x.shape[0] // 8):
            turn = (4 * i - (0 if side == 2 else POS - 4)) % 128
            block = x[8 * i : 8 * i + 8]
            out = jnp.where((place >> 2) == i, pltpu.roll(block, turn, 1) if turn else block, out)
        return out

    def spread_out(x, count, side):
        base = 0 if side == 2 else POS - 4
        out = []
        for i in range(count):
            turn = (base - 4 * i) % 128
            out.append(jnp.where((place >> 2) == base // 4, pltpu.roll(x, turn, 1) if turn else x, 0.0))
        return jnp.concatenate(out)

    def c_copies(app):
        found = []
        for b, col in ((0, west), (2, east), (1, gy)):
            for kind, (row, snd, rcv) in enumerate(((gx, snd_c, snd_c), (north, snd_n, rcv_n), (south, snd_s, rcv_s))):
                if b == 1 and kind == 0:
                    continue
                found.append(
                    pltpu.make_async_remote_copy(
                        src_ref=snd.at[app] if b == 1 else snd_side.at[app, kind, b // 2],
                        dst_ref=rcv.at[app] if b == 1 else rcv_side.at[app, kind, b // 2],
                        send_sem=c_send.at[app, kind, b], recv_sem=c_recv.at[app, kind, b],
                        device_id=(row, col), device_id_type=MESH,
                    )
                )
        return found

    def restrict(app, v):
        wide = dot_right(v, cols_w[...])
        z = dot_left(rows_w[...].astype(BF16), wide) * NINE
        for kind, (start, count, ref) in enumerate(((0, 48, snd_c), (48, 32, snd_n), (80, 32, snd_s))):
            for b in (0, 2):
                snd_side[app, kind, b // 2] = squeeze(z[start : start + count, 128 * b : 128 * (b + 1)], b)
            ref[app] = z[start : start + count, 128:256]

    loads[3].wait()
    loads[4].wait()
    wide = members.shape[-1]
    natural = members[...].astype(F32).reshape(144, wide).astype(BF16)
    shape = (24, 144)
    at = iota(shape, 0)
    zero = jnp.zeros((208, 128), BF16)
    raw[:, 0:128] = zero
    raw[:, 128 + wide : 256 + wide] = zero
    order = []
    for g in range(4):
        for row in range(2):
            value = jnp.where((at < 18) & (iota(shape, 1) == (9 * g + (at >> 1)) * 4 + (at & 1) * 2 + row), 1, 0)
            order.append(value.astype(F32).astype(BF16))
    raw[0:192, 128 : 128 + wide] = jnp.dot(
        jnp.concatenate(order), natural, preferred_element_type=F32
    ).astype(BF16)
    by_lev = rates[...].astype(F32).reshape(4, wide)
    kcomp[0:16] = jnp.zeros((16, 128), F32)
    for tile in range(wide // 128):
        lanes = slice(128 * tile, 128 * (tile + 1))
        for at_row, of in enumerate((0, 2, 1, 3)):
            kcomp[at_row : at_row + 1] = by_lev[of : of + 1, lanes]
        raw[192:208, 128 + 128 * tile : 256 + 128 * tile] = kcomp[0:16].astype(BF16)
    group = iota((24, 128), 1) >> 5
    for odd in range(2):
        shape = (256, 128)
        at = iota(shape, 1)
        from_lane = (128 * (1 - odd) + TC * odd - HC) + 3 * (at & 31) + (at >> 5)
        value = jnp.where(((at & 31) < POS) & (at < 96) & (iota(shape, 0) == from_lane), 1, 0)
        select = value.astype(F32).astype(BF16)
        for j in range(odd, NY, 2):
            lane = 128 * ((j + 1) // 2)
            cut = jnp.dot(raw[:, lane : lane + 256], select, preferred_element_type=F32)
            for row in range(2):
                for p in range(3):
                    x = jnp.zeros((24, 128), F32)
                    for g in range(4):
                        piece = cut[24 * (2 * g + row) : 24 * (2 * g + row + 1)]
                        turn = (32 * (g - p)) % 128
                        x = jnp.where(group == g, pltpu.roll(piece, turn, 1) if turn else piece, x)
                    start = 18 * (3 * row + p)
                    stage[j, start : start + 24] = x
            stage[j, MSG - 4 : MSG] = cut[192:196]
            source[j] = stage[j, 0:MSG].astype(BF16)

    pl.semaphore_wait(barrier, (NX // 4 - 1) + (4 * NY - 1) + 6 + (NY - 1))

    moves = []
    for d in range(1, NY):
        col = lax.rem(gy + d, NY)
        moves.append(
            pltpu.make_async_remote_copy(
                src_ref=source.at[col], dst_ref=mbuf.at[gy + 5],
                send_sem=m_send.at[d], recv_sem=m_recv.at[d],
                device_id=(gx, col), device_id_type=MESH,
            )
        )
    for copy in moves:
        copy.start()
    own = pltpu.make_async_copy(source.at[gy], mbuf.at[gy + 5], m_local)
    own.start()

    has_n = jnp.where(gx > 0, 1, 0)
    has_s = jnp.where(gx < NX - 1, 1, 0)
    has_w = jnp.where(gy > 0, 1, 0)
    has_e = jnp.where(gy < NY - 1, 1, 0)
    for b, on in ((0, has_w), (1, 1), (2, has_e)):
        shape = (FC, 128)
        at = iota(shape, 1)
        cell = 3 * (at & 31) + (at >> 5) - HC + TC * (b - 1)
        value = jnp.where(((at & 31) < POS) & (at < 96), weight(iota(shape, 0), cell) * on, 0)
        cols_w[:, 128 * b : 128 * (b + 1)] = value.astype(F32).astype(BF16)
    for start, count, shift, on in ((0, 24, -2, 1), (48, 16, -2, has_n), (80, 16, 6, has_s)):
        shape = (count, 2 * FR)
        for lev in range(2):
            fine = iota(shape, 1) - FR * lev
            value = jnp.where((fine >= 0) & (fine < FR), weight(fine, iota(shape, 0) + shift) * on, 0)
            rows_w[start + count * lev : start + count * (lev + 1), :] = value.astype(F32)
    loads[0].wait()
    loads[1].wait()
    first = wobs[...] * innov[...]
    vq[0] = first
    restrict(0, first)
    for copy in c_copies(0):
        copy.start()

    shape = (2 * FR, (TR + 2) * 8)
    lev_of = jnp.where(iota(shape, 0) >= FR, 1, 0)
    inner = iota(shape, 1)
    value = jnp.where((inner & 1) == lev_of, weight(iota(shape, 0) - FR * lev_of, (inner >> 3) - 1), 0)
    prows_w[...] = value.astype(F32).astype(BF16)
    for p in range(3):
        shape = (128, FC)
        at = iota(shape, 0) & 31
        value = jnp.where(at < POS, weight(iota(shape, 1), 3 * at + p - HC), 0)
        pcols_w[128 * p : 128 * (p + 1)] = value.astype(F32).astype(BF16)
        shape = (128, 128)
        at = iota(shape, 1) & 31
        value = jnp.where((at < POS) & (iota(shape, 0) == 32 * p + at), 1, 0)
        spread_w[:, 128 * p : 128 * (p + 1)] = value.astype(F32).astype(BF16)

    def halo(side, d):
        g = lax.rem(gy + NY - d, NY)
        return g <= 4 if side == 0 else g >= 3, pltpu.make_async_remote_copy(
            src_ref=source.at[gy] if d == 0 else mbuf.at[g + 5],
            dst_ref=mbuf.at[jnp.minimum(g, 4) + 13 if side == 0 else jnp.maximum(g, 3) - 3],
            send_sem=h_send.at[side, d], recv_sem=h_recv.at[side, d],
            device_id=(north if side == 0 else south, gy), device_id_type=MESH,
        )

    def halo_do(d, what):
        for side in range(2):
            used, copy = halo(side, d)

            @pl.when(used)
            def _():
                getattr(copy, what)()

    halo_do(0, "start")
    for d in range(1, NY):
        moves[d - 1].wait_recv()
        halo_do(d, "start")
    own.wait()

    def unpack(pair):
        unpacked[pair, 0:MSG] = mbuf[pair].astype(F32)
        real = iota((24, 128), 0) < 18
        for row in range(2):
            for p in range(3):
                start = 18 * (3 * row + p)
                x = jnp.where(real, unpacked[pair, start : start + 24], 0.0)
                mf[2 * pair + row, p] = x.reshape(3, 8, 128)
        kcomp[4 * pair : 4 * pair + 4] = unpacked[pair, MSG - 4 : MSG]

    loads[2].wait()
    for pair in range(5, 13):
        unpack(pair)
    for d in range(NY):
        halo_do(d, "wait_recv")
    for pair in (0, 1, 2, 3, 4, 13, 14, 15, 16, 17):
        unpack(pair)

    lev_odd = (iota((8, 128), 0) & 1) == 1
    kw[...] = jnp.dot(kcomp[...].astype(BF16), spread_w[...], preferred_element_type=F32)

    def by_level(ref, even, odd, p):
        lanes = slice(128 * p, 128 * (p + 1))
        return jnp.where(
            lev_odd, jnp.broadcast_to(ref[odd : odd + 1, lanes], (8, 128)), jnp.broadcast_to(ref[even : even + 1, lanes], (8, 128))
        )

    on_n, on_s = jnp.where(gx > 0, 1.0, 0.0), jnp.where(gx < NX - 1, 1.0, 0.0)
    for e in range(ER):
        for p in range(3):
            rate = by_level(kw, 2 * e, 2 * e + 1, p)
            rate = rate * (on_n if e < HR else on_s if e >= HR + TR else 1.0)
            known = rate > 0.0
            kbuf[e, p] = rate
            qbuf[e, p] = 1.0 - 4.0 * rate
            ibuf[e, p] = jnp.where(known, 1.0, 0.0)
            rbuf[e, p] = jnp.where(known, 1.0 / jnp.where(known, rate, 1.0) - 4.0, 0.0)

    def apply(app, v):
        for copy in c_copies(app):
            copy.wait_recv()
        def total(kind, middle):
            count = middle.shape[0] // 8
            sides = [spread_out(rcv_side[app, kind, b // 2], count, b) for b in (0, 2)]
            return middle + (sides[0] + sides[1])

        mine = total(0, snd_c[app])
        north_in = total(2, rcv_s[app])
        south_in = total(1, rcv_n[app])
        for lev in range(2):
            c, n, s = mine[24 * lev : 24 * lev + 24], north_in[16 * lev : 16 * lev + 16], south_in[16 * lev : 16 * lev + 16]
            cbuf[40 * lev + 0 : 40 * lev + 8] = n[0:8]
            cbuf[40 * lev + 8 : 40 * lev + 16] = n[8:16] + c[0:8]
            cbuf[40 * lev + 16 : 40 * lev + 24] = c[8:16]
            cbuf[40 * lev + 24 : 40 * lev + 32] = c[16:24] + s[0:8]
            cbuf[40 * lev + 32 : 40 * lev + 40] = s[8:16]
        cw[...] = dot_right(cbuf[...], spread_w[...])
        for e in range(1, ER - 1):
            for p in range(3):
                kc[e, p] = by_level(cw, e, 40 + e, p) * kbuf[e, p]
        bufs = (xa, xb)
        for t in range(2 * NPASS):
            src, dst = bufs[t % 2], bufs[(t + 1) % 2]

            def row(r, src=src, t=t):
                return [mf[r, p] * kc[r, p][None] if t == 0 else src[r, p] for p in range(3)]

            def store(r, p, x, dst=dst, t=t):
                if t == 2 * NPASS - 1:
                    at = 8 * (r - HR + 1)
                    acc[at : at + 8, 128 * p : 128 * (p + 1)] = jnp.sum(x * mf[r, p], axis=0)
                else:
                    dst[r, p] = x

            middle = t == NPASS - 1
            diffuse(row, store, rbuf if middle else qbuf, ibuf if middle else kbuf, 2 + t, ER - 2 - t)
        tall = dot_left(prows_w[...], acc[...])
        scale = sscale[...]
        return scale * scale * v + dot_right(tall, pcols_w[...]) * NINE

    lane = iota((1, 128), 1)

    def pack(pairs, first=0):
        out = jnp.zeros((1, 128), F32)
        for i, (left, right) in enumerate(pairs):
            total = jnp.sum(jnp.sum(left * right, axis=0, keepdims=True), axis=1, keepdims=True)
            out = jnp.where(lane == i + first, total, out)
        return out

    def y_copy(use, d):
        return pltpu.make_async_remote_copy(
            src_ref=red_own.at[use], dst_ref=red_y.at[use, d], send_sem=ry_send.at[use, d], recv_sem=ry_recv.at[use, d],
            device_id=along_z(d), device_id_type=MESH,
        )

    def x_copy(use, d):
        return pltpu.make_async_remote_copy(
            src_ref=red_own2.at[use], dst_ref=red_x.at[use, d], send_sem=rx_send.at[use, d], recv_sem=rx_recv.at[use, d],
            device_id=in_plane(d), device_id_type=MESH,
        )

    def each(count, make, what):
        def body(d, _):
            getattr(make(d), what)()
            return 0

        lax.fori_loop(1, count, body, 0)

    def reduce_start(use, row):
        red_own[use] = row
        each(NY, functools.partial(y_copy, use), "start")

    def reduce_middle(use):
        each(NY, functools.partial(y_copy, use), "wait_recv")
        total = red_own[use]
        for d in range(1, NY):
            total = total + red_y[use, d]
        red_own2[use] = total
        each(NX, functools.partial(x_copy, use), "start")

    def reduce_end(use):
        each(NX, functools.partial(x_copy, use), "wait_recv")
        total = red_own2[use]
        for d in range(1, NX):
            total = total + red_x[use, d]
        each(NY, functools.partial(y_copy, use), "wait_send")
        each(NX, functools.partial(x_copy, use), "wait_send")
        return total

    def pick(row, i):
        return jnp.sum(jnp.where(lane == i, row, 0.0), axis=1, keepdims=True)

    w = wobs[...]
    b0 = apply(0, vq[0])
    vb[0] = b0
    q1 = w * b0
    restrict(1, q1)
    for copy in c_copies(1):
        copy.start()
    reduce_start(0, pack(((vq[0], b0), (q1, b0))))
    vq[1] = q1
    reduce_middle(0)
    b1 = apply(1, vq[1])
    q2 = w * b1
    restrict(2, q2)
    for copy in c_copies(2):
        copy.start()
    vq[2] = q2
    sums = reduce_end(0)
    theta = pick(sums, 1) / pick(sums, 0)
    last[1] = theta * b1
    q0, b0 = vq[0], vb[0]
    q2 = q2 - theta * vq[1]
    last[0] = q2
    q1 = vq[1] - theta * q0
    vq[1] = q1
    b1 = b1 - theta * b0
    vb[1] = b1
    early = pack(((q0, b0), (q0, b1), (b0, q2), (q1, b1), (b1, q2), (b0, w * b0), (b0, w * b1), (b1, w * b1)))
    b2 = apply(2, vq[2]) - last[1]
    vb[2] = b2
    vq[2] = last[0]
    late = pack(((vq[2], b2), (b2, wobs[...] * b2)), 8)
    row = jnp.where(lane >= 8, late, early)
    reduce_start(1, row)
    reduce_middle(1)
    sums = reduce_end(1)
    e00, e01, e02, e11, e12, f00, f01, f11, e22, f22 = [pick(sums, i) for i in range(10)]
    s00, s01, s02 = e00 + f00, e01 + f01, e02 + (e12 + theta * e02)
    s11, s12, s22 = e11 + f11, e12 + e22, e22 + f22
    tiny = 1e-7
    i0 = 1.0 / s00
    l10, l20 = s01 * i0, s02 * i0
    d1 = s11 - l10 * s01
    i1 = jnp.where(d1 > tiny * s11, 1.0 / d1, 0.0)
    t12 = s12 - l10 * s02
    l21 = t12 * i1
    d2 = s22 - l20 * s02 - l21 * t12
    i2 = jnp.where(d2 > tiny * s22, 1.0 / d2, 0.0)
    r0, r1, r2 = e00, e01, e02
    r1 = r1 - l10 * r0
    r2 = r2 - l20 * r0 - l21 * r1
    z2 = r2 * i2
    z1 = r1 * i1 - l21 * z2
    z0 = r0 * i0 - l10 * z1 - l20 * z2
    inc_ref[...] = z0 * vb[0] + z1 * vb[1] + z2 * vb[2]
    stat_ref[...] = sscale[...] * (z0 * vq[0] + z1 * vq[1] + z2 * vq[2])

    for app in range(3):
        for copy in c_copies(app):
            copy.wait_send()
    for copy in moves:
        copy.wait_send()
    for d in range(NY):
        halo_do(d, "wait_send")


def per_device(NX, NY, innovation, obs_weight, static_scale, members, diffusivity):
    vec = (2 * FR, FC)
    vmem = pl.BlockSpec(memory_space=pltpu.VMEM)
    dma = pltpu.SemaphoreType.DMA
    inc, stat = pl.pallas_call(
        functools.partial(kernel, NX, NY),
        out_shape=(jax.ShapeDtypeStruct(vec, F32), jax.ShapeDtypeStruct(vec, F32)),
        in_specs=[pl.BlockSpec(memory_space=pl.ANY)] * 5,
        out_specs=(vmem, vmem),
        scratch_shapes=[
            pltpu.VMEM(vec, F32),
            pltpu.VMEM(vec, F32),
            pltpu.VMEM(vec, F32),
            pltpu.VMEM(members.shape, BF16),
            pltpu.VMEM(diffusivity.shape, BF16),
            pltpu.VMEM((208, members.shape[-1] + 256), BF16),
            pltpu.VMEM((PAIRS, MSG, 128), BF16),
            pltpu.VMEM((ER, 3, 3, 8, 128), F32),
            pltpu.VMEM((ER, 3, 3, 8, 128), F32),
            pltpu.VMEM((ER, 3, 3, 8, 128), F32),
            pltpu.VMEM((ER, 3, 8, 128), F32),
            pltpu.VMEM((ER, 3, 8, 128), F32),
            pltpu.VMEM((ER, 3, 8, 128), F32),
            pltpu.VMEM((ER, 3, 8, 128), F32),
            pltpu.VMEM((ER, 3, 8, 128), F32),
            pltpu.VMEM(((TR + 2) * 8, 384), F32),
            pltpu.VMEM((80, 128), F32),
            pltpu.VMEM((80, 384), F32),
            pltpu.VMEM((2 * ER, 384), F32),
            pltpu.VMEM((2 * ER, 128), F32),
            pltpu.VMEM((NY, MSG + 8, 128), F32),
            pltpu.VMEM((NY, MSG, 128), BF16),
            pltpu.VMEM((PAIRS, MSG + 8, 128), F32),
            pltpu.VMEM((112, 2 * FR), F32),
            pltpu.VMEM((FC, 384), BF16),
            pltpu.VMEM((2 * FR, (TR + 2) * 8), BF16),
            pltpu.VMEM((384, FC), BF16),
            pltpu.VMEM((128, 384), BF16),
            pltpu.VMEM((3, 48, 128), F32),
            pltpu.VMEM((3, 32, 128), F32),
            pltpu.VMEM((3, 32, 128), F32),
            pltpu.VMEM((3, 3, 2, 8, 128), F32),
            pltpu.VMEM((3, 32, 128), F32),
            pltpu.VMEM((3, 32, 128), F32),
            pltpu.VMEM((3, 3, 2, 8, 128), F32),
            pltpu.VMEM((3,) + vec, F32),
            pltpu.VMEM((3,) + vec, F32),
            pltpu.VMEM((2,) + vec, F32),
            pltpu.VMEM((2, 1, 128), F32),
            pltpu.VMEM((2, NY, 1, 128), F32),
            pltpu.VMEM((2, 1, 128), F32),
            pltpu.VMEM((2, NX, 1, 128), F32),
            dma((5,)), dma((NY,)), dma((NY,)), dma,
            dma((2, NY)), dma((2, NY)),
            dma((3, 3, 3)), dma((3, 3, 3)),
            dma((2, NY)), dma((2, NY)),
            dma((2, NX)), dma((2, NX)),
        ],
        compiler_params=pltpu.CompilerParams(collective_id=0, has_side_effects=True),
        name="solve",
    )(innovation.reshape(vec), obs_weight.reshape(vec), static_scale.reshape(vec), members, diffusivity)
    return inc.reshape(2, FR, FC), stat.reshape(2, FR, FC)


def solution(mesh):
    NX, NY = mesh.shape["gx"], mesh.shape["gy"]
    fine = P(None, "gx", "gy")
    return jax.shard_map(
        functools.partial(per_device, NX, NY),
        mesh=mesh,
        in_specs=(fine, fine, fine, P(None, None, ("gx", "gy"), None), P(None, ("gx", "gy"), None)),
        out_specs=(fine, fine),
        check_vma=False,
    )
```

```python
import functools

import jax
import jax.numpy as jnp
from jax import lax
from jax.experimental import pallas as pl
from jax.experimental.pallas import tpu as pltpu
from jax.sharding import PartitionSpec as P

TR, TC, FR, FC = 16, 64, 48, 192
HR, HC, ER, POS = 10, 9, 36, 28
MSG = 112
PAIRS = ER // 2
NPASS = 4
F32, BF16 = jnp.float32, jnp.bfloat16
MESH = pl.DeviceIdType.MESH
NINE = 1.0 / 9.0


def iota(shape, dim):
    return lax.broadcasted_iota(jnp.int32, shape, dim)


def weight(fine, coarse):
    return jnp.maximum(3 - jnp.abs(fine - 3 * coarse - 1), 0)


def parts(x):
    high = x.astype(BF16)
    return high, (x - high.astype(F32)).astype(BF16)


def dot_left(const, x):
    return functools.reduce(jnp.add, [jnp.dot(const, p, preferred_element_type=F32) for p in parts(x)])


def dot_right(x, const):
    return functools.reduce(jnp.add, [jnp.dot(p, const, preferred_element_type=F32) for p in parts(x)])


def diffuse(row, store, center, around, first, last):
    above, here = row(first - 1), row(first)
    for r in range(first, last):
        below = row(r + 1)
        for p in range(3):
            before = here[p - 1] if p else pltpu.roll(here[2], 1, 2)
            after = here[p + 1] if p < 2 else pltpu.roll(here[0], 127, 2)
            near = (above[p] + below[p]) + (before + after)
            store(r, p, center[r, p][None] * here[p] + around[r, p][None] * near)
        above, here = here, below


def kernel(
    NX, NY, innov_in, wobs_in, sscale_in, members_in, rates_in,
    inc_ref, stat_ref,
    innov, wobs, sscale, members, rates, raw,
    mbuf, mf, xa, xb, kbuf, qbuf, ibuf, rbuf, kc, acc, cbuf, cw, kw, kcomp, stage, source, unpacked,
    rows_w, cols_w, prows_w, pcols_w, spread_w,
    snd_c, snd_n, snd_s, snd_side, rcv_n, rcv_s, rcv_side,
    vq, vb, last, red_own, red_y, red_own2, red_x,
    in_sem, m_send, m_recv, m_local, h_send, h_recv, c_send, c_recv, ry_send, ry_recv, rx_send, rx_recv,
):
    gx, gy = lax.axis_index("gx"), lax.axis_index("gy")
    north, south = lax.rem(gx + NX - 1, NX), lax.rem(gx + 1, NX)
    west, east = lax.rem(gy + NY - 1, NY), lax.rem(gy + 1, NY)

    barrier = pltpu.get_barrier_semaphore()

    def along_z(d):
        z = lax.rem(2 * lax.div(gx, 8) + lax.rem(gy, 2) + d, NX // 4)
        return 8 * lax.div(z, 2) + lax.rem(gx, 8), 2 * lax.div(gy, 2) + lax.rem(z, 2)

    def in_plane(d):
        u = lax.rem(4 * lax.rem(gx, 8) + lax.div(gy, 2) + d, 4 * NY)
        return 8 * lax.div(gx, 8) + lax.div(u, 4), 2 * lax.rem(u, 4) + lax.rem(gy, 2)

    for row in (north, south):
        for col in (west, east, gy):
            pl.semaphore_signal(barrier, inc=1, device_id=(row, col), device_id_type=MESH)
    for d in (4, 3, 5, 2, 6, 1, 7):
        pl.semaphore_signal(barrier, inc=1, device_id=along_z(d), device_id_type=MESH)
    for d in range(1, 4 * NY):
        pl.semaphore_signal(barrier, inc=1, device_id=in_plane(d), device_id_type=MESH)
    for d in range(1, NY):
        pl.semaphore_signal(barrier, inc=1, device_id=(gx, lax.rem(gy + d, NY)), device_id_type=MESH)

    loads = [
        pltpu.make_async_copy(src, dst, in_sem.at[i])
        for i, (src, dst) in enumerate(
            ((innov_in, innov), (wobs_in, wobs), (sscale_in, sscale), (members_in, members), (rates_in, rates))
        )
    ]
    for copy in loads:
        copy.start()

    place = iota((8, 128), 1) & 31

    def squeeze(x, side):
        out = jnp.zeros((8, 128), F32)
        for i in range(x.shape[0] // 8):
            turn = (4 * i - (0 if side == 2 else POS - 4)) % 128
            block = x[8 * i : 8 * i + 8]
            out = jnp.where((place >> 2) == i, pltpu.roll(block, turn, 1) if turn else block, out)
        return out

    def spread_out(x, count, side):
        base = 0 if side == 2 else POS - 4
        out = []
        for i in range(count):
            turn = (base - 4 * i) % 128
            out.append(jnp.where((place >> 2) == base // 4, pltpu.roll(x, turn, 1) if turn else x, 0.0))
        return jnp.concatenate(out)

    def c_copies(app):
        found = []
        for b, col in ((0, west), (2, east), (1, gy)):
            for kind, (row, snd, rcv) in enumerate(((gx, snd_c, snd_c), (north, snd_n, rcv_n), (south, snd_s, rcv_s))):
                if b == 1 and kind == 0:
                    continue
                found.append(
                    pltpu.make_async_remote_copy(
                        src_ref=snd.at[app] if b == 1 else snd_side.at[app, kind, b // 2],
                        dst_ref=rcv.at[app] if b == 1 else rcv_side.at[app, kind, b // 2],
                        send_sem=c_send.at[app, kind, b], recv_sem=c_recv.at[app, kind, b],
                        device_id=(row, col), device_id_type=MESH,
                    )
                )
        return found

    def restrict(app, v):
        wide = dot_right(v, cols_w[...])
        z = dot_left(rows_w[...].astype(BF16), wide) * NINE
        for kind, (start, count, ref) in enumerate(((0, 48, snd_c), (48, 32, snd_n), (80, 32, snd_s))):
            for b in (0, 2):
                snd_side[app, kind, b // 2] = squeeze(z[start : start + count, 128 * b : 128 * (b + 1)], b)
            ref[app] = z[start : start + count, 128:256]

    loads[3].wait()
    loads[4].wait()
    wide = members.shape[-1]
    natural = members[...].astype(F32).reshape(144, wide).astype(BF16)
    shape = (24, 144)
    at = iota(shape, 0)
    zero = jnp.zeros((208, 128), BF16)
    raw[:, 0:128] = zero
    raw[:, 128 + wide : 256 + wide] = zero
    order = []
    for g in range(4):
        for row in range(2):
            value = jnp.where((at < 18) & (iota(shape, 1) == (9 * g + (at >> 1)) * 4 + (at & 1) * 2 + row), 1, 0)
            order.append(value.astype(F32).astype(BF16))
    raw[0:192, 128 : 128 + wide] = jnp.dot(
        jnp.concatenate(order), natural, preferred_element_type=F32
    ).astype(BF16)
    by_lev = rates[...].astype(F32).reshape(4, wide)
    kcomp[0:16] = jnp.zeros((16, 128), F32)
    for tile in range(wide // 128):
        lanes = slice(128 * tile, 128 * (tile + 1))
        for at_row, of in enumerate((0, 2, 1, 3)):
            kcomp[at_row : at_row + 1] = by_lev[of : of + 1, lanes]
        raw[192:208, 128 + 128 * tile : 256 + 128 * tile] = kcomp[0:16].astype(BF16)
    group = iota((24, 128), 1) >> 5
    for odd in range(2):
        shape = (256, 128)
        at = iota(shape, 1)
        from_lane = (128 * (1 - odd) + TC * odd - HC) + 3 * (at & 31) + (at >> 5)
        value = jnp.where(((at & 31) < POS) & (at < 96) & (iota(shape, 0) == from_lane), 1, 0)
        select = value.astype(F32).astype(BF16)
        for j in range(odd, NY, 2):
            lane = 128 * ((j + 1) // 2)
            cut = jnp.dot(raw[:, lane : lane + 256], select, preferred_element_type=F32)
            for row in range(2):
                for p in range(3):
                    x = jnp.zeros((24, 128), F32)
                    for g in range(4):
                        piece = cut[24 * (2 * g + row) : 24 * (2 * g + row + 1)]
                        turn = (32 * (g - p)) % 128
                        x = jnp.where(group == g, pltpu.roll(piece, turn, 1) if turn else piece, x)
                    start = 18 * (3 * row + p)
                    stage[j, start : start + 24] = x
            stage[j, MSG - 4 : MSG] = cut[192:196]
            source[j] = stage[j, 0:MSG].astype(BF16)

    pl.semaphore_wait(barrier, (NX // 4 - 1) + (4 * NY - 1) + 6 + (NY - 1))

    moves = []
    for d in range(1, NY):
        col = lax.rem(gy + d, NY)
        moves.append(
            pltpu.make_async_remote_copy(
                src_ref=source.at[col], dst_ref=mbuf.at[gy + 5],
                send_sem=m_send.at[d], recv_sem=m_recv.at[d],
                device_id=(gx, col), device_id_type=MESH,
            )
        )
    for copy in moves:
        copy.start()
    own = pltpu.make_async_copy(source.at[gy], mbuf.at[gy + 5], m_local)
    own.start()

    has_n = jnp.where(gx > 0, 1, 0)
    has_s = jnp.where(gx < NX - 1, 1, 0)
    has_w = jnp.where(gy > 0, 1, 0)
    has_e = jnp.where(gy < NY - 1, 1, 0)
    for b, on in ((0, has_w), (1, 1), (2, has_e)):
        shape = (FC, 128)
        at = iota(shape, 1)
        cell = 3 * (at & 31) + (at >> 5) - HC + TC * (b - 1)
        value = jnp.where(((at & 31) < POS) & (at < 96), weight(iota(shape, 0), cell) * on, 0)
        cols_w[:, 128 * b : 128 * (b + 1)] = value.astype(F32).astype(BF16)
    for start, count, shift, on in ((0, 24, -2, 1), (48, 16, -2, has_n), (80, 16, 6, has_s)):
        shape = (count, 2 * FR)
        for lev in range(2):
            fine = iota(shape, 1) - FR * lev
            value = jnp.where((fine >= 0) & (fine < FR), weight(fine, iota(shape, 0) + shift) * on, 0)
            rows_w[start + count * lev : start + count * (lev + 1), :] = value.astype(F32)
    loads[0].wait()
    loads[1].wait()
    first = wobs[...] * innov[...]
    vq[0] = first
    restrict(0, first)
    for copy in c_copies(0):
        copy.start()

    shape = (2 * FR, (TR + 2) * 8)
    lev_of = jnp.where(iota(shape, 0) >= FR, 1, 0)
    inner = iota(shape, 1)
    value = jnp.where((inner & 1) == lev_of, weight(iota(shape, 0) - FR * lev_of, (inner >> 3) - 1), 0)
    prows_w[...] = value.astype(F32).astype(BF16)
    for p in range(3):
        shape = (128, FC)
        at = iota(shape, 0) & 31
        value = jnp.where(at < POS, weight(iota(shape, 1), 3 * at + p - HC), 0)
        pcols_w[128 * p : 128 * (p + 1)] = value.astype(F32).astype(BF16)
        shape = (128, 128)
        at = iota(shape, 1) & 31
        value = jnp.where((at < POS) & (iota(shape, 0) == 32 * p + at), 1, 0)
        spread_w[:, 128 * p : 128 * (p + 1)] = value.astype(F32).astype(BF16)

    def halo(side, d):
        g = lax.rem(gy + NY - d, NY)
        return g <= 4 if side == 0 else g >= 3, pltpu.make_async_remote_copy(
            src_ref=source.at[gy] if d == 0 else mbuf.at[g + 5],
            dst_ref=mbuf.at[jnp.minimum(g, 4) + 13 if side == 0 else jnp.maximum(g, 3) - 3],
            send_sem=h_send.at[side, d], recv_sem=h_recv.at[side, d],
            device_id=(north if side == 0 else south, gy), device_id_type=MESH,
        )

    def halo_do(d, what):
        for side in range(2):
            used, copy = halo(side, d)

            @pl.when(used)
            def _():
                getattr(copy, what)()

    halo_do(0, "start")
    for d in range(1, NY):
        moves[d - 1].wait_recv()
        halo_do(d, "start")
    own.wait()

    def unpack(pair):
        unpacked[pair, 0:MSG] = mbuf[pair].astype(F32)
        real = iota((24, 128), 0) < 18
        for row in range(2):
            for p in range(3):
                start = 18 * (3 * row + p)
                x = jnp.where(real, unpacked[pair, start : start + 24], 0.0)
                mf[2 * pair + row, p] = x.reshape(3, 8, 128)
        kcomp[4 * pair : 4 * pair + 4] = unpacked[pair, MSG - 4 : MSG]

    loads[2].wait()
    for pair in range(5, 13):
        unpack(pair)
    for d in range(NY):
        halo_do(d, "wait_recv")
    for pair in (0, 1, 2, 3, 4, 13, 14, 15, 16, 17):
        unpack(pair)

    lev_odd = (iota((8, 128), 0) & 1) == 1
    kw[...] = jnp.dot(kcomp[...].astype(BF16), spread_w[...], preferred_element_type=F32)

    def by_level(ref, even, odd, p):
        lanes = slice(128 * p, 128 * (p + 1))
        return jnp.where(
            lev_odd, jnp.broadcast_to(ref[odd : odd + 1, lanes], (8, 128)), jnp.broadcast_to(ref[even : even + 1, lanes], (8, 128))
        )

    on_n, on_s = jnp.where(gx > 0, 1.0, 0.0), jnp.where(gx < NX - 1, 1.0, 0.0)
    for e in range(ER):
        for p in range(3):
            rate = by_level(kw, 2 * e, 2 * e + 1, p)
            rate = rate * (on_n if e < HR else on_s if e >= HR + TR else 1.0)
            known = rate > 0.0
            kbuf[e, p] = rate
            qbuf[e, p] = 1.0 - 4.0 * rate
            ibuf[e, p] = jnp.where(known, 1.0, 0.0)
            rbuf[e, p] = jnp.where(known, 1.0 / jnp.where(known, rate, 1.0) - 4.0, 0.0)

    def apply(app, v):
        for copy in c_copies(app):
            copy.wait_recv()
        def total(kind, middle):
            count = middle.shape[0] // 8
            sides = [spread_out(rcv_side[app, kind, b // 2], count, b) for b in (0, 2)]
            return middle + (sides[0] + sides[1])

        mine = total(0, snd_c[app])
        north_in = total(2, rcv_s[app])
        south_in = total(1, rcv_n[app])
        for lev in range(2):
            c, n, s = mine[24 * lev : 24 * lev + 24], north_in[16 * lev : 16 * lev + 16], south_in[16 * lev : 16 * lev + 16]
            cbuf[40 * lev + 0 : 40 * lev + 8] = n[0:8]
            cbuf[40 * lev + 8 : 40 * lev + 16] = n[8:16] + c[0:8]
            cbuf[40 * lev + 16 : 40 * lev + 24] = c[8:16]
            cbuf[40 * lev + 24 : 40 * lev + 32] = c[16:24] + s[0:8]
            cbuf[40 * lev + 32 : 40 * lev + 40] = s[8:16]
        cw[...] = dot_right(cbuf[...], spread_w[...])
        for e in range(1, ER - 1):
            for p in range(3):
                kc[e, p] = by_level(cw, e, 40 + e, p) * kbuf[e, p]
        bufs = (xa, xb)
        for t in range(2 * NPASS):
            src, dst = bufs[t % 2], bufs[(t + 1) % 2]

            def row(r, src=src, t=t):
                return [mf[r, p] * kc[r, p][None] if t == 0 else src[r, p] for p in range(3)]

            def store(r, p, x, dst=dst, t=t):
                if t == 2 * NPASS - 1:
                    at = 8 * (r - HR + 1)
                    acc[at : at + 8, 128 * p : 128 * (p + 1)] = jnp.sum(x * mf[r, p], axis=0)
                else:
                    dst[r, p] = x

            middle = t == NPASS - 1
            diffuse(row, store, rbuf if middle else qbuf, ibuf if middle else kbuf, 2 + t, ER - 2 - t)
        tall = dot_left(prows_w[...], acc[...])
        scale = sscale[...]
        return scale * scale * v + dot_right(tall, pcols_w[...]) * NINE

    lane = iota((1, 128), 1)

    def pack(pairs, first=0):
        out = jnp.zeros((1, 128), F32)
        for i, (left, right) in enumerate(pairs):
            total = jnp.sum(jnp.sum(left * right, axis=0, keepdims=True), axis=1, keepdims=True)
            out = jnp.where(lane == i + first, total, out)
        return out

    def y_copy(use, d):
        return pltpu.make_async_remote_copy(
            src_ref=red_own.at[use], dst_ref=red_y.at[use, d], send_sem=ry_send.at[use, d], recv_sem=ry_recv.at[use, d],
            device_id=along_z(d), device_id_type=MESH,
        )

    def x_copy(use, d):
        return pltpu.make_async_remote_copy(
            src_ref=red_own2.at[use], dst_ref=red_x.at[use, d], send_sem=rx_send.at[use, d], recv_sem=rx_recv.at[use, d],
            device_id=in_plane(d), device_id_type=MESH,
        )

    def each(count, make, what):
        def body(d, _):
            getattr(make(d), what)()
            return 0

        lax.fori_loop(1, count, body, 0)

    def reduce_start(use, row):
        red_own[use] = row
        each(NY, functools.partial(y_copy, use), "start")

    def reduce_middle(use):
        each(NY, functools.partial(y_copy, use), "wait_recv")
        total = red_own[use]
        for d in range(1, NY):
            total = total + red_y[use, d]
        red_own2[use] = total
        each(NX, functools.partial(x_copy, use), "start")

    def reduce_end(use):
        each(NX, functools.partial(x_copy, use), "wait_recv")
        total = red_own2[use]
        for d in range(1, NX):
            total = total + red_x[use, d]
        each(NY, functools.partial(y_copy, use), "wait_send")
        each(NX, functools.partial(x_copy, use), "wait_send")
        return total

    def pick(row, i):
        return jnp.sum(jnp.where(lane == i, row, 0.0), axis=1, keepdims=True)

    w = wobs[...]
    b0 = apply(0, vq[0])
    vb[0] = b0
    q1 = w * b0
    restrict(1, q1)
    for copy in c_copies(1):
        copy.start()
    reduce_start(0, pack(((vq[0], b0), (q1, b0))))
    vq[1] = q1
    reduce_middle(0)
    b1 = apply(1, vq[1])
    q2 = w * b1
    restrict(2, q2)
    for copy in c_copies(2):
        copy.start()
    vq[2] = q2
    sums = reduce_end(0)
    theta = pick(sums, 1) / pick(sums, 0)
    last[1] = theta * b1
    q0, b0 = vq[0], vb[0]
    q2 = q2 - theta * vq[1]
    last[0] = q2
    q1 = vq[1] - theta * q0
    vq[1] = q1
    b1 = b1 - theta * b0
    vb[1] = b1
    early = pack(((q0, b0), (q0, b1), (b0, q2), (q1, b1), (b1, q2), (b0, w * b0), (b0, w * b1), (b1, w * b1)))
    b2 = apply(2, vq[2]) - last[1]
    vb[2] = b2
    vq[2] = last[0]
    late = pack(((vq[2], b2), (b2, wobs[...] * b2)), 8)
    row = jnp.where(lane >= 8, late, early)
    reduce_start(1, row)
    reduce_middle(1)
    sums = reduce_end(1)
    e00, e01, e02, e11, e12, f00, f01, f11, e22, f22 = [pick(sums, i) for i in range(10)]
    s00, s01, s02 = e00 + f00, e01 + f01, e02 + (e12 + theta * e02)
    s11, s12, s22 = e11 + f11, e12 + e22, e22 + f22
    tiny = 1e-7
    i0 = 1.0 / s00
    l10, l20 = s01 * i0, s02 * i0
    d1 = s11 - l10 * s01
    i1 = jnp.where(d1 > tiny * s11, 1.0 / d1, 0.0)
    t12 = s12 - l10 * s02
    l21 = t12 * i1
    d2 = s22 - l20 * s02 - l21 * t12
    i2 = jnp.where(d2 > tiny * s22, 1.0 / d2, 0.0)
    r0, r1, r2 = e00, e01, e02
    r1 = r1 - l10 * r0
    r2 = r2 - l20 * r0 - l21 * r1
    z2 = r2 * i2
    z1 = r1 * i1 - l21 * z2
    z0 = r0 * i0 - l10 * z1 - l20 * z2
    inc_ref[...] = z0 * vb[0] + z1 * vb[1] + z2 * vb[2]
    stat_ref[...] = sscale[...] * (z0 * vq[0] + z1 * vq[1] + z2 * vq[2])

    for app in range(3):
        for copy in c_copies(app):
            copy.wait_send()
    for copy in moves:
        copy.wait_send()
    for d in range(NY):
        halo_do(d, "wait_send")


def per_device(NX, NY, innovation, obs_weight, static_scale, members, diffusivity):
    vec = (2 * FR, FC)
    vmem = pl.BlockSpec(memory_space=pltpu.VMEM)
    dma = pltpu.SemaphoreType.DMA
    inc, stat = pl.pallas_call(
        functools.partial(kernel, NX, NY),
        out_shape=(jax.ShapeDtypeStruct(vec, F32), jax.ShapeDtypeStruct(vec, F32)),
        in_specs=[pl.BlockSpec(memory_space=pl.ANY)] * 5,
        out_specs=(vmem, vmem),
        scratch_shapes=[
            pltpu.VMEM(vec, F32),
            pltpu.VMEM(vec, F32),
            pltpu.VMEM(vec, F32),
            pltpu.VMEM(members.shape, BF16),
            pltpu.VMEM(diffusivity.shape, BF16),
            pltpu.VMEM((208, members.shape[-1] + 256), BF16),
            pltpu.VMEM((PAIRS, MSG, 128), BF16),
            pltpu.VMEM((ER, 3, 3, 8, 128), F32),
            pltpu.VMEM((ER, 3, 3, 8, 128), F32),
            pltpu.VMEM((ER, 3, 3, 8, 128), F32),
            pltpu.VMEM((ER, 3, 8, 128), F32),
            pltpu.VMEM((ER, 3, 8, 128), F32),
            pltpu.VMEM((ER, 3, 8, 128), F32),
            pltpu.VMEM((ER, 3, 8, 128), F32),
            pltpu.VMEM((ER, 3, 8, 128), F32),
            pltpu.VMEM(((TR + 2) * 8, 384), F32),
            pltpu.VMEM((80, 128), F32),
            pltpu.VMEM((80, 384), F32),
            pltpu.VMEM((2 * ER, 384), F32),
            pltpu.VMEM((2 * ER, 128), F32),
            pltpu.VMEM((NY, MSG + 8, 128), F32),
            pltpu.VMEM((NY, MSG, 128), BF16),
            pltpu.VMEM((PAIRS, MSG + 8, 128), F32),
            pltpu.VMEM((112, 2 * FR), F32),
            pltpu.VMEM((FC, 384), BF16),
            pltpu.VMEM((2 * FR, (TR + 2) * 8), BF16),
            pltpu.VMEM((384, FC), BF16),
            pltpu.VMEM((128, 384), BF16),
            pltpu.VMEM((3, 48, 128), F32),
            pltpu.VMEM((3, 32, 128), F32),
            pltpu.VMEM((3, 32, 128), F32),
            pltpu.VMEM((3, 3, 2, 8, 128), F32),
            pltpu.VMEM((3, 32, 128), F32),
            pltpu.VMEM((3, 32, 128), F32),
            pltpu.VMEM((3, 3, 2, 8, 128), F32),
            pltpu.VMEM((3,) + vec, F32),
            pltpu.VMEM((3,) + vec, F32),
            pltpu.VMEM((2,) + vec, F32),
            pltpu.VMEM((2, 1, 128), F32),
            pltpu.VMEM((2, NY, 1, 128), F32),
            pltpu.VMEM((2, 1, 128), F32),
            pltpu.VMEM((2, NX, 1, 128), F32),
            dma((5,)), dma((NY,)), dma((NY,)), dma,
            dma((2, NY)), dma((2, NY)),
            dma((3, 3, 3)), dma((3, 3, 3)),
            dma((2, NY)), dma((2, NY)),
            dma((2, NX)), dma((2, NX)),
        ],
        compiler_params=pltpu.CompilerParams(collective_id=0, has_side_effects=True),
        name="solve",
    )(innovation.reshape(vec), obs_weight.reshape(vec), static_scale.reshape(vec), members, diffusivity)
    return inc.reshape(2, FR, FC), stat.reshape(2, FR, FC)


def solution(mesh):
    NX, NY = mesh.shape["gx"], mesh.shape["gy"]
    fine = P(None, "gx", "gy")
    return jax.shard_map(
        functools.partial(per_device, NX, NY),
        mesh=mesh,
        in_specs=(fine, fine, fine, P(None, None, ("gx", "gy"), None), P(None, ("gx", "gy"), None)),
        out_specs=(fine, fine),
        check_vma=False,
    )
```
